128 devices in a mesh: sys: 8 (over x, core), slab: 16 (over z, y).
Axes of the slice: x: 4, y: 4, z: 4, core: 2. Of those that a mesh axis runs over, the one named last changes fastest.
Arguments:
- right_side: float32 [256, 1024, 128], P('slab', 'sys'), parts along dimension 1, may hold values from -8 to 8
- diagonal: float32 [256, 1024, 128], P('slab', 'sys'), parts along dimension 1, may hold values from 0.25 to 2
Outputs:
- solution_field: float32 [256, 1024, 128], P('slab', 'sys'), parts along dimension 1
- residual: float32 [256, 1024, 128], P('slab', 'sys'), parts along dimension 1
The draws below stay inside these ranges and needn't reach their ends.
There are 8 independent parts, one for each index of `sys`. The reference program is written for one: setup_inputs(seed, part) draws one part's arguments, and reference() takes and returns one part's arrays. A program takes and returns all parts, laid end to end along the dimension named above; each array names one. Nothing has to cross between parts.
All inputs are finite; a program needn't handle non-finite values.
Results may differ from the reference program's by a relative error of at most 0.0003.
Values sent between devices are 32-bit elements; how exact they have to be, the bound alone decides.
A program may use at most 64 MiB of HBM per device.

```python
import math
import jax
import jax.numpy as jnp

NY = 128
NX = 128
ITERS = 10
NZ = 256


def draw_right_side(key, part):
    depth_index = jnp.arange(NZ, dtype=jnp.float32)
    scales = 3.0 ** (depth_index / max(NZ - 1, 1))
    values = jax.random.normal(key, (NZ, NY, NX), jnp.float32)
    return jnp.clip(values * scales[:, None, None], -8.0, 8.0)


def levels(rng, dims, shards, smallest, largest):
    level = 1.0
    for dim, blocks in shards:
        steps = jax.random.uniform(jax.random.fold_in(jax.random.fold_in(rng, 6), dim), (blocks,), jnp.float32, smallest / len(shards), largest / len(shards))
        level = level * jnp.repeat(jnp.exp(steps), dims[dim] // blocks).reshape((-1,) + (1,) * (len(dims) - 1 - dim))
    return level


def setup_inputs(seed: int = 0, part: int = 0) -> dict:
    splits = jax.random.split(jax.random.key(seed), 3)
    own_keys = jax.random.split(jax.random.fold_in(splits[2], part), 3)
    right_side = draw_right_side(jax.random.fold_in(jax.random.fold_in(splits[2], part), 71), part)
    diagonal = jnp.clip(jnp.exp(math.log(2.0) - 2.0794415 * jax.random.uniform(own_keys[1], (NZ, NY, NX), jnp.float32) ** levels(own_keys[1], (NZ, NY, NX), ((0, 16),), -0.2, 0.2)), 0.25, 2.0)
    return {"right_side": right_side, "diagonal": diagonal}


def operate(values, diagonal):
    padded = jnp.pad(values, 1)
    beside = padded[2:, 1:-1, 1:-1] + padded[:-2, 1:-1, 1:-1]
    beside = beside + padded[1:-1, 2:, 1:-1] + padded[1:-1, :-2, 1:-1]
    beside = beside + padded[1:-1, 1:-1, 2:] + padded[1:-1, 1:-1, :-2]
    return (6.0 + diagonal) * values - beside


def reference(right_side, diagonal):
    solution_field = jnp.zeros_like(right_side)
    residual = right_side
    direction = right_side
    norm_now = jnp.sum(residual * residual)
    for iteration in range(ITERS):
        applied = operate(direction, diagonal)
        step_size = norm_now / jnp.sum(direction * applied)
        solution_field = solution_field + step_size * direction
        residual = residual - step_size * applied
        norm_next = jnp.sum(residual * residual)
        direction = residual + (norm_next / norm_now) * direction
        norm_now = norm_next
    return solution_field, residual
```

```python
import functools

import jax
import jax.numpy as jnp
import numpy as np
from jax import lax
from jax.experimental import pallas as pl
from jax.experimental.pallas import tpu as pltpu
from jax.sharding import PartitionSpec as P

MID = 7.125
HALF = 6.875
BLOCKS = (3, 3, 4)
STEPS = sum(BLOCKS)
BASES = tuple(int(b) for b in np.cumsum((0,) + BLOCKS[:-1]))
GHOST = max(BLOCKS)
PAD = 8
SLOTS = 8
SHIFT = 32
MESH = pl.DeviceIdType.MESH


def tables():
    n = STEPS
    apply = np.zeros((n + 1, n))
    at_zero = np.zeros(n + 1)
    at_zero[0] = 1.0
    for base, steps in zip(BASES, BLOCKS):
        for j in range(steps):
            i = base + j
            apply[i, i] = MID
            if j == 0:
                apply[i + 1, i] = HALF
                at_zero[i + 1] = -MID / HALF * at_zero[i]
            else:
                apply[i + 1, i] = apply[i - 1, i] = HALF / 2
                at_zero[i + 1] = -2 * MID / HALF * at_zero[i] - at_zero[i - 1]
    divide = np.zeros((n, n + 1))
    divide[:, 1:] = -np.linalg.inv(apply[1:])
    maps = np.concatenate([divide, np.eye(n + 1), at_zero[None]]).T
    sides = np.zeros((24, 128))
    sides[:n, SHIFT : SHIFT + maps.shape[1]] = -maps[:n]
    sides[16:, SHIFT : SHIFT + maps.shape[1]] = maps[n]
    high = sides.astype(np.float32)
    return np.stack([high, (sides - high).astype(np.float32)])


def two_sum(a, b):
    s = a + b
    t = s - a
    return s, (a - (s - t)) + (b - t)


def quick(a, b):
    s = a + b
    return s, b - (s - a)


def halves(a):
    c = a * 4097.0
    h = c - (c - a)
    return h, a - h


def add2(a, b):
    s, e = two_sum(a[0], b[0])
    return quick(s, e + (a[1] + b[1]))


def mul2(a, b):
    p = a[0] * b[0]
    ah, al = halves(a[0])
    bh, bl = halves(b[0])
    e = ((ah * bh - p) + (ah * bl + al * bh)) + al * bl
    return quick(p, e + (a[0] * b[1] + a[1] * b[0]))


def neg2(a):
    return (-a[0], -a[1])


def inverse2(a):
    y = 1.0 / a[0]
    zero = jnp.zeros_like(y)
    p, e = mul2(a, (y, zero))
    return quick(y, y * ((1.0 - p) - e))


def tree2(parts):
    while len(parts) > 1:
        parts = [add2(parts[i], parts[i + 1]) for i in range(0, len(parts) - 1, 2)] + (
            [parts[-1]] if len(parts) % 2 else []
        )
    return parts[0]


def sublanes2(a):
    for shift in (4, 2, 1):
        a = add2(a, tuple(pltpu.roll(v, shift, 0) for v in a))
    return a


def kernel(
    devices,
    right_ref,
    diag_ref,
    table_ref,
    x_ref,
    r_ref,
    V,
    D,
    ACC,
    RED,
    PACK,
    SEND,
    GOT,
    TAB,
    load_sem,
    send_sem,
    recv_sem,
    all_send,
    all_recv,
    store_sem,
):
    planes, rows = right_ref.shape[0], right_ref.shape[1]
    chunks = rows // 8
    me = lax.axis_index("slab")
    below = lax.rem(me + devices - 1, devices)
    above = lax.rem(me + 1, devices)
    has_below = me > 0
    has_above = me < devices - 1
    body = pl.ds(PAD, rows)
    deep = GHOST

    def load(ref, at, first, count, sem):
        return pltpu.make_async_copy(
            ref.at[pl.ds(first, count)], at.at[pl.ds(GHOST + first, count), body], load_sem.at[sem]
        )

    loads = []
    for sem, (ref, at) in enumerate(((right_ref, V.at[0]), (diag_ref, D))):
        loads.append(load(ref, at, 0, deep, 3 * sem))
        loads.append(load(ref, at, planes - deep, deep, 3 * sem + 1))
    for sem, (ref, at) in enumerate(((right_ref, V.at[0]), (diag_ref, D))):
        loads.append(load(ref, at, deep, planes - 2 * deep, 3 * sem + 2))
    table_load = pltpu.make_async_copy(table_ref, TAB, load_sem.at[6])
    for copy in loads:
        copy.start()
    table_load.start()

    barrier = pltpu.get_barrier_semaphore()
    for o in range(1, devices):
        pl.semaphore_signal(
            barrier, inc=1, device_id={"slab": lax.rem(me + o, devices)}, device_id_type=MESH
        )

    zero = jnp.zeros((8, 128), jnp.float32)

    def clear(i, _):
        for k in range(STEPS):
            V[k, i, 0:8, :] = zero
            V[k, i, PAD + rows : PAD + rows + 8, :] = zero
        return 0

    lax.fori_loop(0, planes + 2 * GHOST, clear, 0)

    def clear_ghost(first):
        for base in BASES:
            for i in range(GHOST):
                for c in range(chunks):
                    V[base, first + i, PAD + 8 * c : PAD + 8 * c + 8, :] = zero

    @pl.when(jnp.logical_not(has_below))
    def _():
        clear_ghost(0)

    @pl.when(jnp.logical_not(has_above))
    def _():
        clear_ghost(GHOST + planes)

    def message(array, plane, up, t):
        if up:
            source, target = GHOST + planes - 1 - plane, GHOST - 1 - plane
        else:
            source, target = GHOST + plane, GHOST + planes + plane
        return pltpu.make_async_remote_copy(
            src_ref=array.at[source, body],
            dst_ref=array.at[target, body],
            send_sem=send_sem.at[int(up), t],
            recv_sem=recv_sem.at[int(up), t],
            device_id={"slab": above if up else below},
            device_id_type=MESH,
        )

    numbers = {}
    order = []
    diag_sent = 0
    for index, (base, steps) in enumerate(zip(BASES, BLOCKS)):
        for plane in range(steps):
            order.append((index, "v", plane))
            if index == 0 and plane < steps - 1:
                order.append((index, "d", plane))
        upto = steps - 1 if index + 1 == len(BLOCKS) else max(BLOCKS[: index + 2]) - 1
        for plane in range(max(diag_sent, BLOCKS[0] - 1), upto):
            order.append((index, "d", plane))
        diag_sent = max(upto, diag_sent, BLOCKS[0] - 1)
    for t, (index, kind, plane) in enumerate(order):
        numbers[(kind, plane) if kind == "d" else (kind, index, plane)] = t

    def of(index, kind, plane, up):
        t = numbers[(kind, plane) if kind == "d" else (kind, index, plane)]
        return message(D if kind == "d" else V.at[BASES[index]], plane, up, t)

    def send_round(index):
        for which, kind, plane in order:
            if which == index:

                @pl.when(has_below)
                def _(kind=kind, plane=plane):
                    of(index, kind, plane, False).start()

                @pl.when(has_above)
                def _(kind=kind, plane=plane):
                    of(index, kind, plane, True).start()

    def receive(index, kind, plane):
        @pl.when(has_below)
        def _():
            of(index, kind, plane, True).wait_recv()

        @pl.when(has_above)
        def _():
            of(index, kind, plane, False).wait_recv()

    lane = lax.broadcasted_iota(jnp.int32, (8, 128), 1)
    leftmost, rightmost = lane == 0, lane == 127
    scale = np.float32(2.0 / HALF)

    def scale_diag(first, count):
        def one(i, _):
            for c in range(chunks):
                at = pl.ds(PAD + 8 * c, 8)
                D[first + i, at, :] = (D[first + i, at, :] + np.float32(6.0 - MID)) * scale
            return 0

        lax.fori_loop(0, count, one, 0)

    def step(source, target, before, plane, keep=None):
        for c in range(chunks):
            at = pl.ds(PAD + 8 * c, 8)
            v = V[source, plane, at, :]
            sides = (V[source, plane - 1, at, :] + V[source, plane + 1, at, :]) + (
                V[source, plane, pl.ds(PAD + 8 * c - 1, 8), :]
                + V[source, plane, pl.ds(PAD + 8 * c + 1, 8), :]
            )
            sides = sides + (
                jnp.where(leftmost, 0.0, pltpu.roll(v, 1, 1))
                + jnp.where(rightmost, 0.0, pltpu.roll(v, 127, 1))
            )
            new = D[plane, at, :] * v - scale * sides
            new = 0.5 * new if before is None else new - V[before, plane, at, :]
            V[target, plane, at, :] = new if keep is None else jnp.where(keep, new, 0.0)

    def inner(base, steps):
        for j in range(1, steps + 1):
            before = None if j == 1 else base + j - 2

            def pair(i, _, j=j, before=before):
                first = GHOST + j + 2 * i
                step(base + j - 1, base + j, before, first)
                step(base + j - 1, base + j, before, first + 1)
                return 0

            lax.fori_loop(0, (planes - 2 * j) // 2, pair, 0)

    def wave(base, steps, g):
        low, high = GHOST - g, GHOST + planes - 1 + g

        def one(j, before):
            keep_low = jnp.logical_or(has_below, j >= g)
            keep_high = jnp.logical_or(has_above, j >= g)
            step(base + j - 1, base + j, before, low + j, keep_low)
            step(base + j - 1, base + j, before, high - j, keep_high)

        one(1, None)

        def later(j, _):
            one(j, base + j - 2)
            return 0

        lax.fori_loop(2, steps + 1, later, 0)

    pairs = [(i, j) for j in range(STEPS + 1) for i in range(j + 1)]
    place = {pair: i for i, pair in enumerate(pairs)}

    def products(first, last, two, slot):
        mine = [p for p in pairs if first <= p[1] <= last and p != (STEPS, STEPS)]

        def add(plane):
            def some(c, acc):
                acc = list(acc)
                for u in range(2):
                    at = pl.ds(pl.multiple_of(PAD + 16 * c + 8 * u, 8), 8)
                    v = [V[k, plane, at, :] for k in range(last + 1)]
                    for a, (i, j) in enumerate(mine):
                        acc[a] = acc[a] + v[i] * v[j]
                return tuple(acc)

            return some

        acc = tuple(zero for _ in mine)
        for plane in two:
            acc = lax.fori_loop(0, chunks // 2, add(plane), acc)
        for value, pair in zip(acc, mine):
            ACC[place[pair], slot] = value

    def all_products(first, last):
        def one(slot, _):
            products(first, last, (GHOST + 2 * slot, GHOST + 2 * slot + 1), slot)
            return 0

        lax.fori_loop(0, planes // 2, one, 0)

    def reduce(where, count):
        for pair, lanes in where.items():
            value = (ACC[place[pair], 0], zero)
            for slot in range(1, SLOTS):
                s, e = two_sum(value[0], ACC[place[pair], slot])
                value = (s, value[1] + e)
            for n in lanes:
                RED[0, 8 * n : 8 * n + 8, :] = value[0]
                RED[1, 8 * n : 8 * n + 8, :] = value[1]
        for q in range(16):
            if 8 * q >= count:
                PACK[0, 8 * q : 8 * q + 8, :] = zero
                PACK[1, 8 * q : 8 * q + 8, :] = zero
                continue
            total = tree2(
                [
                    tuple(RED[h, pl.ds(64 * q + s, 8, stride=8), :] for h in range(2))
                    for s in range(8)
                ]
            )
            PACK[0, 8 * q : 8 * q + 8, :] = total[0]
            PACK[1, 8 * q : 8 * q + 8, :] = total[1]
        high, low = jnp.transpose(PACK[0]), jnp.transpose(PACK[1])
        total = sublanes2(
            tree2([(high[8 * q : 8 * q + 8], low[8 * q : 8 * q + 8]) for q in range(16)])
        )
        return total

    def spread(k, o):
        return pltpu.make_async_remote_copy(
            src_ref=SEND.at[k],
            dst_ref=GOT.at[k, me],
            send_sem=all_send.at[k, o],
            recv_sem=all_recv.at[k, me],
            device_id={"slab": lax.rem(me + o, devices)},
            device_id_type=MESH,
        )

    def arrival(k, o):
        source = lax.rem(me + o, devices)
        return pltpu.make_async_remote_copy(
            src_ref=SEND.at[k],
            dst_ref=GOT.at[k, source],
            send_sem=all_send.at[k, o],
            recv_sem=all_recv.at[k, source],
            device_id={"slab": source},
            device_id_type=MESH,
        )

    def share(k, total):
        SEND[k, 0:1, :] = total[0][0:1]
        SEND[k, 1:2, :] = total[1][0:1]
        GOT[k, me, 0:1, :] = total[0][0:1]
        GOT[k, me, 1:2, :] = total[1][0:1]
        for o in range(1, devices):
            spread(k, o).start()

    def collect(k):
        for o in range(1, devices):
            arrival(k, o).wait_recv()
        value = (GOT[k, 0], jnp.zeros((2, 128), jnp.float32))
        for d in range(1, devices):
            s, e = two_sum(value[0], GOT[k, d])
            value = (s, value[1] + e)
        high = jnp.broadcast_to(value[0][0:1], (8, 128))
        low = jnp.broadcast_to(value[1][0:1] + value[0][1:2], (8, 128))
        return quick(high, low)

    for copy in loads[:4]:
        copy.wait()
    scale_diag(GHOST, deep)
    scale_diag(GHOST + planes - deep, deep)
    pl.semaphore_wait(barrier, devices - 1)
    send_round(0)
    for copy in loads[4:]:
        copy.wait()
    scale_diag(GHOST + deep, planes - 2 * deep)

    n = STEPS
    last_base, last_steps = BASES[-1], BLOCKS[-1]
    for index, (base, steps) in enumerate(zip(BASES, BLOCKS)):
        final = index + 1 == len(BLOCKS)
        if index > 0:
            send_round(index)
            all_products(BASES[index - 1] + 1 if index > 1 else 0, base)
        inner(base, steps)
        if final:

            def early(slot, _):
                at = GHOST + last_steps - 1 + 2 * slot
                products(base + 1, n - 1, (at, at + 1), slot)
                return 0

            def late(slot, _):
                at = GHOST + last_steps + 2 * slot
                products(n, n, (at, at + 1), slot)
                return 0

            lax.fori_loop(0, planes // 2 - last_steps + 1, early, 0)
            lax.fori_loop(0, planes // 2 - last_steps, late, 0)
        for g in range(1, steps + 1):
            receive(index, "v", g - 1)
            if g > 1 and ("d", g - 2) in numbers:
                which = order[numbers[("d", g - 2)]][0]
                if which == index or (index > 0 and which == index - 1 and g - 1 >= BLOCKS[index - 1]):
                    receive(which, "d", g - 2)
            wave(base, steps, g)
            if final:
                if g < steps:
                    near = steps - 1 - g
                    products(
                        base + 1,
                        n - 1,
                        (GHOST + near, GHOST + planes - 1 - near),
                        planes // 2 - steps + g,
                    )
                near = steps - g
                products(n, n, (GHOST + near, GHOST + planes - 1 - near), planes // 2 - steps + g - 1)
                if g == steps - 1:
                    where = {
                        (i, j): sorted({n * i + j, n * j + i}) for i, j in pairs if j < n
                    }
                    share(0, reduce(where, n * n))
    share(1, reduce({(i, n): [i] for i in range(n)}, n))

    table_load.wait()
    sub = lax.broadcasted_iota(jnp.int32, (8, 128), 0)
    got = collect(0)
    parts = []
    for h in range(2):
        top, bottom = zero, zero
        for i in range(n):
            moved = got[h] if i == 0 else pltpu.roll(got[h], 128 - n * i, 1)
            if i < 8:
                top = jnp.where(sub == i, moved, top)
            else:
                bottom = jnp.where(sub == i - 8, moved, bottom)
        both = jnp.concatenate([top, bottom], axis=0)
        wide = lax.broadcasted_iota(jnp.int32, (16, 128), 1)
        parts.append(jnp.where(wide < n, both, TAB[h, 0:16, :]))
    M = tuple(parts)
    row = lax.broadcasted_iota(jnp.int32, (16, 128), 0)
    for k in range(n):
        column = tuple(jnp.broadcast_to(m[:, k : k + 1], (16, 128)) for m in M)
        pivot = tuple(jnp.broadcast_to(c[k : k + 1, :], (16, 128)) for c in column)
        scaled = mul2(tuple(jnp.broadcast_to(m[k : k + 1, :], (16, 128)) for m in M), inverse2(pivot))
        rest = add2(M, neg2(mul2(column, scaled)))
        M = tuple(jnp.where(row == k, s, m) for s, m in zip(scaled, rest))
    got = collect(1)
    wide = lax.broadcasted_iota(jnp.int32, (16, 128), 1)
    H = tuple(
        jnp.broadcast_to(
            jnp.sum(
                jnp.where(wide == row, jnp.concatenate([v, v], axis=0), 0.0), axis=1, keepdims=True
            ),
            (16, 128),
        )
        for v in got
    )
    H = tuple(jnp.where(row < n, v, 0.0) for v in H)
    M = tuple(jnp.where(row < n, m, 0.0) for m in M)
    terms = mul2(M, H)
    terms = sublanes2(add2(tuple(t[0:8] for t in terms), tuple(t[8:16] for t in terms)))
    terms = add2(terms, (TAB[0, 16:24, :], TAB[1, 16:24, :]))
    value = tuple(
        jnp.broadcast_to(t[:, SHIFT + 2 * n + 1 : SHIFT + 2 * n + 2], (8, 128)) for t in terms
    )
    terms = mul2(terms, inverse2(value))
    factor = terms[0]
    fx = [jnp.broadcast_to(factor[:, SHIFT + i : SHIFT + i + 1], (8, 128)) for i in range(n)]
    fr = [
        jnp.broadcast_to(factor[:, SHIFT + n + i : SHIFT + n + i + 1], (8, 128))
        for i in range(n + 1)
    ]

    for index, kind, plane in order:

        @pl.when(has_below)
        def _(index=index, kind=kind, plane=plane):
            of(index, kind, plane, False).wait_send()

        @pl.when(has_above)
        def _(index=index, kind=kind, plane=plane):
            of(index, kind, plane, True).wait_send()

    stores = []
    group = 4
    for q in range(planes // group):

        def one(i, _, q=q):
            plane = GHOST + group * q + i
            for c in range(chunks):
                at = pl.ds(PAD + 8 * c, 8)
                v = [V[k, plane, at, :] for k in range(n + 1)]
                V[0, plane, at, :] = functools.reduce(jnp.add, [f * u for f, u in zip(fx, v)])
                V[1, plane, at, :] = functools.reduce(jnp.add, [f * u for f, u in zip(fr, v)])
            return 0

        lax.fori_loop(0, group, one, 0)
        for k, out in enumerate((x_ref, r_ref)):
            copy = pltpu.make_async_copy(
                V.at[k, pl.ds(GHOST + group * q, group), body],
                out.at[pl.ds(group * q, group)],
                store_sem.at[k, q],
            )
            copy.start()
            stores.append(copy)

    for k in range(2):
        for o in range(1, devices):
            spread(k, o).wait_send()
    for copy in stores:
        copy.wait()


def local(right_side, diagonal):
    planes, rows, lanes = right_side.shape
    devices = lax.axis_size("slab")
    count = 64
    tall = planes + 2 * GHOST
    f32 = jnp.float32
    out = jax.ShapeDtypeStruct(right_side.shape, f32)
    dma = pltpu.SemaphoreType.DMA
    return pl.pallas_call(
        functools.partial(kernel, devices),
        out_shape=(out, out),
        in_specs=[pl.BlockSpec(memory_space=pl.ANY)] * 3,
        out_specs=(pl.BlockSpec(memory_space=pl.ANY),) * 2,
        scratch_shapes=[
            pltpu.VMEM((STEPS + 1, tall, rows + 2 * PAD, lanes), f32),
            pltpu.VMEM((tall, rows + 2 * PAD, lanes), f32),
            pltpu.VMEM(((STEPS + 1) * (STEPS + 2) // 2, SLOTS, 8, 128), f32),
            pltpu.VMEM((2, 1024, 128), f32),
            pltpu.VMEM((2, 128, 128), f32),
            pltpu.VMEM((2, 2, 128), f32),
            pltpu.VMEM((2, devices, 2, 128), f32),
            pltpu.VMEM((2, 24, 128), f32),
            dma((7,)),
            dma((2, count)),
            dma((2, count)),
            dma((2, devices)),
            dma((2, devices)),
            dma((2, planes // 4)),
        ],
        compiler_params=pltpu.CompilerParams(collective_id=0, has_side_effects=True),
        name="cg",
    )(right_side, diagonal, jnp.asarray(tables()))


def solution(mesh):
    placed = (P("slab", "sys", None), P("slab", "sys", None))
    return jax.shard_map(
        local,
        mesh=mesh,
        in_specs=placed,
        out_specs=placed,
        check_vma=False,
    )
```

```python
import functools

import jax
import jax.numpy as jnp
import numpy as np
from jax import lax
from jax.experimental import pallas as pl
from jax.experimental.pallas import tpu as pltpu
from jax.sharding import PartitionSpec as P

MID = 7.125
HALF = 6.875
BLOCKS = (3, 3, 4)
STEPS = sum(BLOCKS)
BASES = tuple(int(b) for b in np.cumsum((0,) + BLOCKS[:-1]))
GHOST = max(BLOCKS)
PAD = 8
SLOTS = 8
SHIFT = 32
MESH = pl.DeviceIdType.MESH


def tables():
    n = STEPS
    apply = np.zeros((n + 1, n))
    at_zero = np.zeros(n + 1)
    at_zero[0] = 1.0
    for base, steps in zip(BASES, BLOCKS):
        for j in range(steps):
            i = base + j
            apply[i, i] = MID
            if j == 0:
                apply[i + 1, i] = HALF
                at_zero[i + 1] = -MID / HALF * at_zero[i]
            else:
                apply[i + 1, i] = apply[i - 1, i] = HALF / 2
                at_zero[i + 1] = -2 * MID / HALF * at_zero[i] - at_zero[i - 1]
    divide = np.zeros((n, n + 1))
    divide[:, 1:] = -np.linalg.inv(apply[1:])
    maps = np.concatenate([divide, np.eye(n + 1), at_zero[None]]).T
    sides = np.zeros((24, 128))
    sides[:n, SHIFT : SHIFT + maps.shape[1]] = -maps[:n]
    sides[16:, SHIFT : SHIFT + maps.shape[1]] = maps[n]
    high = sides.astype(np.float32)
    return np.stack([high, (sides - high).astype(np.float32)])


def two_sum(a, b):
    s = a + b
    t = s - a
    return s, (a - (s - t)) + (b - t)


def quick(a, b):
    s = a + b
    return s, b - (s - a)


def halves(a):
    c = a * 4097.0
    h = c - (c - a)
    return h, a - h


def add2(a, b):
    s, e = two_sum(a[0], b[0])
    return quick(s, e + (a[1] + b[1]))


def mul2(a, b):
    p = a[0] * b[0]
    ah, al = halves(a[0])
    bh, bl = halves(b[0])
    e = ((ah * bh - p) + (ah * bl + al * bh)) + al * bl
    return quick(p, e + (a[0] * b[1] + a[1] * b[0]))


def neg2(a):
    return (-a[0], -a[1])


def inverse2(a):
    y = 1.0 / a[0]
    zero = jnp.zeros_like(y)
    p, e = mul2(a, (y, zero))
    return quick(y, y * ((1.0 - p) - e))


def tree2(parts):
    while len(parts) > 1:
        parts = [add2(parts[i], parts[i + 1]) for i in range(0, len(parts) - 1, 2)] + (
            [parts[-1]] if len(parts) % 2 else []
        )
    return parts[0]


def sublanes2(a):
    for shift in (4, 2, 1):
        a = add2(a, tuple(pltpu.roll(v, shift, 0) for v in a))
    return a


def kernel(
    devices,
    right_ref,
    diag_ref,
    table_ref,
    x_ref,
    r_ref,
    V,
    D,
    ACC,
    RED,
    PACK,
    SEND,
    GOT,
    TAB,
    load_sem,
    send_sem,
    recv_sem,
    all_send,
    all_recv,
):
    planes, rows = right_ref.shape[0], right_ref.shape[1]
    chunks = rows // 8
    me = lax.axis_index("slab")
    below = lax.rem(me + devices - 1, devices)
    above = lax.rem(me + 1, devices)
    has_below = me > 0
    has_above = me < devices - 1
    body = pl.ds(PAD, rows)
    deep = GHOST

    def load(ref, at, first, count, sem):
        return pltpu.make_async_copy(
            ref.at[pl.ds(first, count)], at.at[pl.ds(GHOST + first, count), body], load_sem.at[sem]
        )

    loads = []
    for sem, (ref, at) in enumerate(((right_ref, V.at[0]), (diag_ref, D))):
        loads.append(load(ref, at, 0, deep, 3 * sem))
        loads.append(load(ref, at, planes - deep, deep, 3 * sem + 1))
    for sem, (ref, at) in enumerate(((right_ref, V.at[0]), (diag_ref, D))):
        loads.append(load(ref, at, deep, planes - 2 * deep, 3 * sem + 2))
    table_load = pltpu.make_async_copy(table_ref, TAB, load_sem.at[6])
    for copy in loads:
        copy.start()
    table_load.start()

    barrier = pltpu.get_barrier_semaphore()
    for o in range(1, devices):
        pl.semaphore_signal(
            barrier, inc=1, device_id={"slab": lax.rem(me + o, devices)}, device_id_type=MESH
        )

    zero = jnp.zeros((8, 128), jnp.float32)

    def clear(i, _):
        for k in range(STEPS):
            V[k, i, 0:8, :] = zero
            V[k, i, PAD + rows : PAD + rows + 8, :] = zero
        return 0

    lax.fori_loop(0, planes + 2 * GHOST, clear, 0)

    def clear_ghost(first):
        for base in BASES:
            for i in range(GHOST):
                for c in range(chunks):
                    V[base, first + i, PAD + 8 * c : PAD + 8 * c + 8, :] = zero

    @pl.when(jnp.logical_not(has_below))
    def _():
        clear_ghost(0)

    @pl.when(jnp.logical_not(has_above))
    def _():
        clear_ghost(GHOST + planes)

    def message(array, plane, up, t):
        if up:
            source, target = GHOST + planes - 1 - plane, GHOST - 1 - plane
        else:
            source, target = GHOST + plane, GHOST + planes + plane
        return pltpu.make_async_remote_copy(
            src_ref=array.at[source, body],
            dst_ref=array.at[target, body],
            send_sem=send_sem.at[int(up), t],
            recv_sem=recv_sem.at[int(up), t],
            device_id={"slab": above if up else below},
            device_id_type=MESH,
        )

    numbers = {}
    order = []
    diag_sent = 0
    for index, (base, steps) in enumerate(zip(BASES, BLOCKS)):
        for plane in range(steps):
            order.append((index, "v", plane))
            if index == 0 and plane < steps - 1:
                order.append((index, "d", plane))
        upto = steps - 1 if index + 1 == len(BLOCKS) else max(BLOCKS[: index + 2]) - 1
        for plane in range(max(diag_sent, BLOCKS[0] - 1), upto):
            order.append((index, "d", plane))
        diag_sent = max(upto, diag_sent, BLOCKS[0] - 1)
    for t, (index, kind, plane) in enumerate(order):
        numbers[(kind, plane) if kind == "d" else (kind, index, plane)] = t

    def of(index, kind, plane, up):
        t = numbers[(kind, plane) if kind == "d" else (kind, index, plane)]
        return message(D if kind == "d" else V.at[BASES[index]], plane, up, t)

    def send_round(index):
        for which, kind, plane in order:
            if which == index:

                @pl.when(has_below)
                def _(kind=kind, plane=plane):
                    of(index, kind, plane, False).start()

                @pl.when(has_above)
                def _(kind=kind, plane=plane):
                    of(index, kind, plane, True).start()

    def receive(index, kind, plane):
        @pl.when(has_below)
        def _():
            of(index, kind, plane, True).wait_recv()

        @pl.when(has_above)
        def _():
            of(index, kind, plane, False).wait_recv()

    lane = lax.broadcasted_iota(jnp.int32, (8, 128), 1)
    leftmost, rightmost = lane == 0, lane == 127
    scale = np.float32(2.0 / HALF)

    def scale_diag(first, count):
        def one(i, _):
            for c in range(chunks):
                at = pl.ds(PAD + 8 * c, 8)
                D[first + i, at, :] = (D[first + i, at, :] + np.float32(6.0 - MID)) * scale
            return 0

        lax.fori_loop(0, count, one, 0)

    def step(source, target, before, plane, keep=None):
        for c in range(chunks):
            at = pl.ds(PAD + 8 * c, 8)
            v = V[source, plane, at, :]
            sides = (V[source, plane - 1, at, :] + V[source, plane + 1, at, :]) + (
                V[source, plane, pl.ds(PAD + 8 * c - 1, 8), :]
                + V[source, plane, pl.ds(PAD + 8 * c + 1, 8), :]
            )
            sides = sides + (
                jnp.where(leftmost, 0.0, pltpu.roll(v, 1, 1))
                + jnp.where(rightmost, 0.0, pltpu.roll(v, 127, 1))
            )
            new = D[plane, at, :] * v - scale * sides
            new = 0.5 * new if before is None else new - V[before, plane, at, :]
            V[target, plane, at, :] = new if keep is None else jnp.where(keep, new, 0.0)

    def inner(base, steps):
        for j in range(1, steps + 1):
            before = None if j == 1 else base + j - 2

            def pair(i, _, j=j, before=before):
                first = GHOST + j + 2 * i
                step(base + j - 1, base + j, before, first)
                step(base + j - 1, base + j, before, first + 1)
                return 0

            lax.fori_loop(0, (planes - 2 * j) // 2, pair, 0)

    def wave(base, steps, g):
        low, high = GHOST - g, GHOST + planes - 1 + g

        def one(j, before):
            keep_low, keep_high = (None, None) if j >= g else (has_below, has_above)
            step(base + j - 1, base + j, before, low + j, keep_low)
            step(base + j - 1, base + j, before, high - j, keep_high)

        for j in range(1, steps + 1):
            one(j, None if j == 1 else base + j - 2)

    pairs = [(i, j) for j in range(STEPS + 1) for i in range(j + 1)]
    place = {pair: i for i, pair in enumerate(pairs)}

    def products(first, last, two, slot):
        mine = [p for p in pairs if first <= p[1] <= last and p != (STEPS, STEPS)]

        def add(plane):
            def some(c, acc):
                acc = list(acc)
                for u in range(4):
                    at = pl.ds(pl.multiple_of(PAD + 32 * c + 8 * u, 8), 8)
                    v = [V[k, plane, at, :] for k in range(last + 1)]
                    for a, (i, j) in enumerate(mine):
                        acc[a] = acc[a] + v[i] * v[j]
                return tuple(acc)

            return some

        acc = tuple(zero for _ in mine)
        for plane in two:
            acc = lax.fori_loop(0, chunks // 4, add(plane), acc)
        for value, pair in zip(acc, mine):
            ACC[place[pair], slot] = value

    def all_products(first, last):
        def one(slot, _):
            products(first, last, (GHOST + 2 * slot, GHOST + 2 * slot + 1), slot)
            return 0

        lax.fori_loop(0, planes // 2, one, 0)

    def reduce(where, count):
        for pair, lanes in where.items():
            value = (ACC[place[pair], 0], zero)
            for slot in range(1, SLOTS):
                s, e = two_sum(value[0], ACC[place[pair], slot])
                value = (s, value[1] + e)
            for n in lanes:
                RED[0, 8 * n : 8 * n + 8, :] = value[0]
                RED[1, 8 * n : 8 * n + 8, :] = value[1]
        for q in range(16):
            if 8 * q >= count:
                PACK[0, 8 * q : 8 * q + 8, :] = zero
                PACK[1, 8 * q : 8 * q + 8, :] = zero
                continue
            total = tree2(
                [
                    tuple(RED[h, pl.ds(64 * q + s, 8, stride=8), :] for h in range(2))
                    for s in range(8)
                ]
            )
            PACK[0, 8 * q : 8 * q + 8, :] = total[0]
            PACK[1, 8 * q : 8 * q + 8, :] = total[1]
        high, low = jnp.transpose(PACK[0]), jnp.transpose(PACK[1])
        total = sublanes2(
            tree2([(high[8 * q : 8 * q + 8], low[8 * q : 8 * q + 8]) for q in range(16)])
        )
        return total

    def spread(k, o):
        return pltpu.make_async_remote_copy(
            src_ref=SEND.at[k],
            dst_ref=GOT.at[k, me],
            send_sem=all_send.at[k, o],
            recv_sem=all_recv.at[k, me],
            device_id={"slab": lax.rem(me + o, devices)},
            device_id_type=MESH,
        )

    def arrival(k, o):
        source = lax.rem(me + o, devices)
        return pltpu.make_async_remote_copy(
            src_ref=SEND.at[k],
            dst_ref=GOT.at[k, source],
            send_sem=all_send.at[k, o],
            recv_sem=all_recv.at[k, source],
            device_id={"slab": source},
            device_id_type=MESH,
        )

    def share(k, total):
        SEND[k, 0:1, :] = total[0][0:1]
        SEND[k, 1:2, :] = total[1][0:1]
        GOT[k, me, 0:1, :] = total[0][0:1]
        GOT[k, me, 1:2, :] = total[1][0:1]
        for o in range(1, devices):
            spread(k, o).start()

    def collect(k):
        for o in range(1, devices):
            arrival(k, o).wait_recv()
        value = (GOT[k, 0], jnp.zeros((2, 128), jnp.float32))
        for d in range(1, devices):
            s, e = two_sum(value[0], GOT[k, d])
            value = (s, value[1] + e)
        high = jnp.broadcast_to(value[0][0:1], (8, 128))
        low = jnp.broadcast_to(value[1][0:1] + value[0][1:2], (8, 128))
        return quick(high, low)

    for copy in loads[:4]:
        copy.wait()
    scale_diag(GHOST, deep)
    scale_diag(GHOST + planes - deep, deep)
    pl.semaphore_wait(barrier, devices - 1)
    send_round(0)
    for copy in loads[4:]:
        copy.wait()
    scale_diag(GHOST + deep, planes - 2 * deep)

    n = STEPS
    last_base, last_steps = BASES[-1], BLOCKS[-1]
    for index, (base, steps) in enumerate(zip(BASES, BLOCKS)):
        final = index + 1 == len(BLOCKS)
        if index > 0:
            send_round(index)
            all_products(BASES[index - 1] + 1 if index > 1 else 0, base)
        inner(base, steps)
        if final:

            def early(slot, _):
                at = GHOST + last_steps - 1 + 2 * slot
                products(base + 1, n - 1, (at, at + 1), slot)
                return 0

            def late(slot, _):
                at = GHOST + last_steps + 2 * slot
                products(n, n, (at, at + 1), slot)
                return 0

            lax.fori_loop(0, planes // 2 - last_steps + 1, early, 0)
            lax.fori_loop(0, planes // 2 - last_steps, late, 0)
        for g in range(1, steps + 1):
            receive(index, "v", g - 1)
            if g > 1 and ("d", g - 2) in numbers:
                which = order[numbers[("d", g - 2)]][0]
                if which == index or (index > 0 and which == index - 1 and g - 1 >= BLOCKS[index - 1]):
                    receive(which, "d", g - 2)
            wave(base, steps, g)
            if final:
                if g < steps:
                    near = steps - 1 - g
                    products(
                        base + 1,
                        n - 1,
                        (GHOST + near, GHOST + planes - 1 - near),
                        planes // 2 - steps + g,
                    )
                near = steps - g
                products(n, n, (GHOST + near, GHOST + planes - 1 - near), planes // 2 - steps + g - 1)
                if g == steps - 1:
                    where = {
                        (i, j): sorted({n * i + j, n * j + i}) for i, j in pairs if j < n
                    }
                    share(0, reduce(where, n * n))
    share(1, reduce({(i, n): [i] for i in range(n)}, n))
    for index, kind, plane in order:

        @pl.when(has_below)
        def _(index=index, kind=kind, plane=plane):
            of(index, kind, plane, False).wait_send()

        @pl.when(has_above)
        def _(index=index, kind=kind, plane=plane):
            of(index, kind, plane, True).wait_send()

    for k in range(2):
        for o in range(1, devices):
            spread(k, o).wait_send()

    table_load.wait()
    sub = lax.broadcasted_iota(jnp.int32, (8, 128), 0)
    got = collect(0)
    parts = []
    for h in range(2):
        top, bottom = zero, zero
        for i in range(n):
            moved = got[h] if i == 0 else pltpu.roll(got[h], 128 - n * i, 1)
            if i < 8:
                top = jnp.where(sub == i, moved, top)
            else:
                bottom = jnp.where(sub == i - 8, moved, bottom)
        both = jnp.concatenate([top, bottom], axis=0)
        wide = lax.broadcasted_iota(jnp.int32, (16, 128), 1)
        parts.append(jnp.where(wide < n, both, TAB[h, 0:16, :]))
    M = tuple(parts)
    row = lax.broadcasted_iota(jnp.int32, (16, 128), 0)
    for k in range(n):
        column = tuple(jnp.broadcast_to(m[:, k : k + 1], (16, 128)) for m in M)
        pivot = tuple(jnp.broadcast_to(c[k : k + 1, :], (16, 128)) for c in column)
        scaled = mul2(tuple(jnp.broadcast_to(m[k : k + 1, :], (16, 128)) for m in M), inverse2(pivot))
        rest = add2(M, neg2(mul2(column, scaled)))
        M = tuple(jnp.where(row == k, s, m) for s, m in zip(scaled, rest))
    got = collect(1)
    wide = lax.broadcasted_iota(jnp.int32, (16, 128), 1)
    H = tuple(
        jnp.broadcast_to(
            jnp.sum(
                jnp.where(wide == row, jnp.concatenate([v, v], axis=0), 0.0), axis=1, keepdims=True
            ),
            (16, 128),
        )
        for v in got
    )
    H = tuple(jnp.where(row < n, v, 0.0) for v in H)
    M = tuple(jnp.where(row < n, m, 0.0) for m in M)
    terms = mul2(M, H)
    terms = sublanes2(add2(tuple(t[0:8] for t in terms), tuple(t[8:16] for t in terms)))
    terms = add2(terms, (TAB[0, 16:24, :], TAB[1, 16:24, :]))
    value = tuple(
        jnp.broadcast_to(t[:, SHIFT + 2 * n + 1 : SHIFT + 2 * n + 2], (8, 128)) for t in terms
    )
    terms = mul2(terms, inverse2(value))
    factor = terms[0]
    fx = [jnp.broadcast_to(factor[:, SHIFT + i : SHIFT + i + 1], (8, 128)) for i in range(n)]
    fr = [
        jnp.broadcast_to(factor[:, SHIFT + n + i : SHIFT + n + i + 1], (8, 128))
        for i in range(n + 1)
    ]

    def one(i, _):
        plane = GHOST + i
        for c in range(chunks):
            at = pl.ds(PAD + 8 * c, 8)
            v = [V[k, plane, at, :] for k in range(n + 1)]
            x_ref[i, 8 * c : 8 * c + 8, :] = functools.reduce(jnp.add, [f * u for f, u in zip(fx, v)])
            r_ref[i, 8 * c : 8 * c + 8, :] = functools.reduce(jnp.add, [f * u for f, u in zip(fr, v)])
        return 0

    lax.fori_loop(0, planes, one, 0)


def store_kernel(x_ref, r_ref, x_out, r_out, sem):
    group = x_ref.shape[0] // 4
    copies = []
    for q in range(4):
        for k, (source, target) in enumerate(((x_ref, x_out), (r_ref, r_out))):
            at = pl.ds(group * q, group)
            copies.append(pltpu.make_async_copy(source.at[at], target.at[at], sem.at[k, q]))
            copies[-1].start()
    for copy in copies:
        copy.wait()


def local(right_side, diagonal):
    planes, rows, lanes = right_side.shape
    devices = lax.axis_size("slab")
    count = 64
    tall = planes + 2 * GHOST
    f32 = jnp.float32
    out = jax.ShapeDtypeStruct(right_side.shape, f32)
    held = pltpu.VMEM(right_side.shape, f32)
    dma = pltpu.SemaphoreType.DMA
    results = pl.pallas_call(
        functools.partial(kernel, devices),
        out_shape=(held, held),
        in_specs=[pl.BlockSpec(memory_space=pltpu.HBM)] * 3,
        out_specs=(pl.BlockSpec(memory_space=pltpu.VMEM),) * 2,
        scratch_shapes=[
            pltpu.VMEM((STEPS + 1, tall, rows + 2 * PAD, lanes), f32),
            pltpu.VMEM((tall, rows + 2 * PAD, lanes), f32),
            pltpu.VMEM(((STEPS + 1) * (STEPS + 2) // 2, SLOTS, 8, 128), f32),
            pltpu.VMEM((2, 1024, 128), f32),
            pltpu.VMEM((2, 128, 128), f32),
            pltpu.VMEM((2, 2, 128), f32),
            pltpu.VMEM((2, devices, 2, 128), f32),
            pltpu.VMEM((2, 24, 128), f32),
            dma((7,)),
            dma((2, count)),
            dma((2, count)),
            dma((2, devices)),
            dma((2, devices)),
        ],
        compiler_params=pltpu.CompilerParams(
            collective_id=0, has_side_effects=True, vmem_limit_bytes=40 * 2**20
        ),
        name="cg",
    )(
        *(
            pltpu.with_memory_space_constraint(a, pltpu.HBM)
            for a in (right_side, diagonal, jnp.asarray(tables()))
        )
    )
    return pl.pallas_call(
        store_kernel,
        out_shape=(out, out),
        in_specs=[pl.BlockSpec(memory_space=pltpu.VMEM)] * 2,
        out_specs=(pl.BlockSpec(memory_space=pltpu.HBM),) * 2,
        scratch_shapes=[dma((2, 4))],
        name="store",
    )(*(pltpu.with_memory_space_constraint(a, pltpu.VMEM) for a in results))


def solution(mesh):
    placed = (P("slab", "sys", None), P("slab", "sys", None))
    return jax.shard_map(
        local,
        mesh=mesh,
        in_specs=placed,
        out_specs=placed,
        check_vma=False,
    )
```

```python
import functools

import jax
import jax.numpy as jnp
import numpy as np
from jax import lax
from jax.experimental import pallas as pl
from jax.experimental.pallas import tpu as pltpu
from jax.sharding import PartitionSpec as P

MID = 7.125
HALF = 6.875
BLOCKS = (3, 3, 4)
STEPS = sum(BLOCKS)
BASES = tuple(int(b) for b in np.cumsum((0,) + BLOCKS[:-1]))
GHOST = max(BLOCKS)
MESSAGES = STEPS + GHOST - 1
PAD = 8
SLOTS = 8
SHIFT = 32
MESH = pl.DeviceIdType.MESH


def tables():
    n = STEPS
    apply = np.zeros((n + 1, n))
    at_zero = np.zeros(n + 1)
    at_zero[0] = 1.0
    for base, steps in zip(BASES, BLOCKS):
        for j in range(steps):
            i = base + j
            apply[i, i] = MID
            if j == 0:
                apply[i + 1, i] = HALF
                at_zero[i + 1] = -MID / HALF * at_zero[i]
            else:
                apply[i + 1, i] = apply[i - 1, i] = HALF / 2
                at_zero[i + 1] = -2 * MID / HALF * at_zero[i] - at_zero[i - 1]
    divide = np.zeros((n, n + 1))
    divide[:, 1:] = -np.linalg.inv(apply[1:])
    maps = np.concatenate([divide, np.eye(n + 1), at_zero[None]]).T
    sides = np.zeros((24, 128))
    sides[:n, SHIFT : SHIFT + maps.shape[1]] = -maps[:n]
    sides[16:, SHIFT : SHIFT + maps.shape[1]] = maps[n]
    high = sides.astype(np.float32)
    return np.stack([high, (sides - high).astype(np.float32)])


def two_sum(a, b):
    s = a + b
    t = s - a
    return s, (a - (s - t)) + (b - t)


def quick(a, b):
    s = a + b
    return s, b - (s - a)


def halves(a):
    c = a * 4097.0
    h = c - (c - a)
    return h, a - h


def add2(a, b):
    s, e = two_sum(a[0], b[0])
    return quick(s, e + (a[1] + b[1]))


def mul2(a, b):
    p = a[0] * b[0]
    ah, al = halves(a[0])
    bh, bl = halves(b[0])
    e = ((ah * bh - p) + (ah * bl + al * bh)) + al * bl
    return quick(p, e + (a[0] * b[1] + a[1] * b[0]))


def neg2(a):
    return (-a[0], -a[1])


def inverse2(a):
    y = 1.0 / a[0]
    zero = jnp.zeros_like(y)
    p, e = mul2(a, (y, zero))
    return quick(y, y * ((1.0 - p) - e))


def tree2(parts):
    while len(parts) > 1:
        parts = [add2(parts[i], parts[i + 1]) for i in range(0, len(parts) - 1, 2)] + (
            [parts[-1]] if len(parts) % 2 else []
        )
    return parts[0]


def sublanes2(a):
    for shift in (4, 2, 1):
        a = add2(a, tuple(pltpu.roll(v, shift, 0) for v in a))
    return a


def kernel(
    devices,
    right_ref,
    diag_ref,
    table_ref,
    x_ref,
    r_ref,
    V,
    D,
    ACC,
    RED,
    PACK,
    SEND,
    GOT,
    TAB,
    load_sem,
    send_sem,
    recv_sem,
    all_send,
    all_recv,
):
    planes, rows = right_ref.shape[0], right_ref.shape[1]
    chunks = rows // 8
    me = lax.axis_index("slab")
    below = lax.rem(me + devices - 1, devices)
    above = lax.rem(me + 1, devices)
    has_below = me > 0
    has_above = me < devices - 1
    body = pl.ds(PAD, rows)
    deep = GHOST

    def load(ref, at, first, count, sem):
        return pltpu.make_async_copy(
            ref.at[pl.ds(first, count)], at.at[pl.ds(GHOST + first, count), body], load_sem.at[sem]
        )

    loads = []
    for sem, (ref, at) in enumerate(((right_ref, V.at[0]), (diag_ref, D))):
        loads.append(load(ref, at, 0, deep, 3 * sem))
        loads.append(load(ref, at, planes - deep, deep, 3 * sem + 1))
    for sem, (ref, at) in enumerate(((right_ref, V.at[0]), (diag_ref, D))):
        loads.append(load(ref, at, deep, planes - 2 * deep, 3 * sem + 2))
    table_load = pltpu.make_async_copy(table_ref, TAB, load_sem.at[6])
    for copy in loads:
        copy.start()
    table_load.start()

    barrier = pltpu.get_barrier_semaphore()
    for o in range(1, devices):
        pl.semaphore_signal(
            barrier, inc=1, device_id={"slab": lax.rem(me + o, devices)}, device_id_type=MESH
        )

    zero = jnp.zeros((8, 128), jnp.float32)

    def clear(i, _):
        for k in range(STEPS):
            V[k, i, 0:8, :] = zero
            V[k, i, PAD + rows : PAD + rows + 8, :] = zero
        return 0

    lax.fori_loop(0, planes + 2 * GHOST, clear, 0)

    def clear_ghost(first):
        for base in BASES:
            for i in range(GHOST):
                for c in range(chunks):
                    V[base, first + i, PAD + 8 * c : PAD + 8 * c + 8, :] = zero

    @pl.when(jnp.logical_not(has_below))
    def _():
        clear_ghost(0)

    @pl.when(jnp.logical_not(has_above))
    def _():
        clear_ghost(GHOST + planes)

    def message(array, plane, up, t):
        if up:
            source, target = GHOST + planes - 1 - plane, GHOST - 1 - plane
        else:
            source, target = GHOST + plane, GHOST + planes + plane
        return pltpu.make_async_remote_copy(
            src_ref=array.at[source, body],
            dst_ref=array.at[target, body],
            send_sem=send_sem.at[int(up)],
            recv_sem=recv_sem.at[int(up), t],
            device_id={"slab": above if up else below},
            device_id_type=MESH,
        )

    numbers = {}
    order = []
    diag_sent = 0
    for index, (base, steps) in enumerate(zip(BASES, BLOCKS)):
        for plane in range(steps):
            order.append((index, "v", plane))
            if index == 0 and plane < steps - 1:
                order.append((index, "d", plane))
        upto = steps - 1 if index + 1 == len(BLOCKS) else max(BLOCKS[: index + 2]) - 1
        for plane in range(max(diag_sent, BLOCKS[0] - 1), upto):
            order.append((index, "d", plane))
        diag_sent = max(upto, diag_sent, BLOCKS[0] - 1)
    for t, (index, kind, plane) in enumerate(order):
        numbers[(kind, plane) if kind == "d" else (kind, index, plane)] = t

    def of(index, kind, plane, up):
        t = numbers[(kind, plane) if kind == "d" else (kind, index, plane)]
        return message(D if kind == "d" else V.at[BASES[index]], plane, up, t)

    def send(index, kind, plane):
        @pl.when(has_below)
        def _():
            of(index, kind, plane, False).start()

        @pl.when(has_above)
        def _():
            of(index, kind, plane, True).start()

    def wait_sent():
        for up, there in ((False, has_below), (True, has_above)):

            @pl.when(there)
            def _(up=up):
                sent = D.at[pl.ds(0, len(order)), body]
                pltpu.make_async_copy(sent, sent, send_sem.at[int(up)]).wait()

    def receive(index, kind, plane):
        @pl.when(has_below)
        def _():
            of(index, kind, plane, True).wait_recv()

        @pl.when(has_above)
        def _():
            of(index, kind, plane, False).wait_recv()

    lane = lax.broadcasted_iota(jnp.int32, (8, 128), 1)
    leftmost, rightmost = lane == 0, lane == 127
    scale = np.float32(2.0 / HALF)

    def scale_diag(first, count):
        def one(i, _):
            for c in range(chunks):
                at = pl.ds(PAD + 8 * c, 8)
                D[first + i, at, :] = (D[first + i, at, :] + np.float32(6.0 - MID)) * scale
            return 0

        lax.fori_loop(0, count, one, 0)

    def step(source, target, before, plane, keep=None):
        for c in range(chunks):
            at = pl.ds(PAD + 8 * c, 8)
            v = V[source, plane, at, :]
            sides = (V[source, plane - 1, at, :] + V[source, plane + 1, at, :]) + (
                V[source, plane, pl.ds(PAD + 8 * c - 1, 8), :]
                + V[source, plane, pl.ds(PAD + 8 * c + 1, 8), :]
            )
            sides = sides + (
                jnp.where(leftmost, 0.0, pltpu.roll(v, 1, 1))
                + jnp.where(rightmost, 0.0, pltpu.roll(v, 127, 1))
            )
            new = D[plane, at, :] * v - scale * sides
            new = 0.5 * new if before is None else new - V[before, plane, at, :]
            V[target, plane, at, :] = new if keep is None else jnp.where(keep, new, 0.0)

    def inner(base, steps):
        for j in range(1, steps + 1):
            before = None if j == 1 else base + j - 2

            def pair(i, _, j=j, before=before):
                first = GHOST + j + 2 * i
                step(base + j - 1, base + j, before, first)
                step(base + j - 1, base + j, before, first + 1)
                return 0

            lax.fori_loop(0, (planes - 2 * j) // 2, pair, 0)

    def wave(base, steps, g):
        low, high = GHOST - g, GHOST + planes - 1 + g

        def one(j, before):
            keep_low, keep_high = (None, None) if j >= g else (has_below, has_above)
            step(base + j - 1, base + j, before, low + j, keep_low)
            step(base + j - 1, base + j, before, high - j, keep_high)

        for j in range(1, steps + 1):
            one(j, None if j == 1 else base + j - 2)

    pairs = [(i, j) for j in range(STEPS + 1) for i in range(j + 1)]
    place = {pair: i for i, pair in enumerate(pairs)}

    def products(first, last, two, slot):
        mine = [p for p in pairs if first <= p[1] <= last and p != (STEPS, STEPS)]

        def add(plane):
            def some(c, acc):
                acc = list(acc)
                for u in range(4):
                    at = pl.ds(pl.multiple_of(PAD + 32 * c + 8 * u, 8), 8)
                    v = [V[k, plane, at, :] for k in range(last + 1)]
                    for a, (i, j) in enumerate(mine):
                        acc[a] = acc[a] + v[i] * v[j]
                return tuple(acc)

            return some

        acc = tuple(zero for _ in mine)
        for plane in two:
            acc = lax.fori_loop(0, chunks // 4, add(plane), acc)
        for value, pair in zip(acc, mine):
            ACC[place[pair], slot] = value

    def inner_products(first, last, near):
        def one(slot, _):
            at = GHOST + near + 2 * slot
            products(first, last, (at, at + 1), slot)
            return 0

        lax.fori_loop(0, planes // 2 - near, one, 0)

    def outer_products(first, last, near):
        def one(i, _):
            products(first, last, (GHOST + i, GHOST + planes - 1 - i), planes // 2 - near + i)
            return 0

        lax.fori_loop(0, near, one, 0)

    def reduce(where, count):
        for pair, lanes in where.items():
            value = (ACC[place[pair], 0], zero)
            for slot in range(1, SLOTS):
                s, e = two_sum(value[0], ACC[place[pair], slot])
                value = (s, value[1] + e)
            for n in lanes:
                RED[0, 8 * n : 8 * n + 8, :] = value[0]
                RED[1, 8 * n : 8 * n + 8, :] = value[1]
        for q in range(16):
            if 8 * q >= count:
                PACK[0, 8 * q : 8 * q + 8, :] = zero
                PACK[1, 8 * q : 8 * q + 8, :] = zero
                continue
            total = tree2(
                [
                    tuple(RED[h, pl.ds(64 * q + s, 8, stride=8), :] for h in range(2))
                    for s in range(8)
                ]
            )
            PACK[0, 8 * q : 8 * q + 8, :] = total[0]
            PACK[1, 8 * q : 8 * q + 8, :] = total[1]
        high, low = jnp.transpose(PACK[0]), jnp.transpose(PACK[1])
        total = sublanes2(
            tree2([(high[8 * q : 8 * q + 8], low[8 * q : 8 * q + 8]) for q in range(16)])
        )
        return total

    def spread(k, o):
        return pltpu.make_async_remote_copy(
            src_ref=SEND.at[k],
            dst_ref=GOT.at[k, me],
            send_sem=all_send.at[k],
            recv_sem=all_recv.at[k],
            device_id={"slab": lax.rem(me + o, devices)},
            device_id_type=MESH,
        )

    def share(k, total):
        SEND[k, 0:1, :] = total[0][0:1]
        SEND[k, 1:2, :] = total[1][0:1]
        GOT[k, me, 0:1, :] = total[0][0:1]
        GOT[k, me, 1:2, :] = total[1][0:1]
        for o in range(1, devices):
            spread(k, o).start()

    def wait_shared():
        for k in range(2):
            sent = GOT.at[k, pl.ds(0, devices - 1)]
            pltpu.make_async_copy(sent, sent, all_send.at[k]).wait()

    def wait_row(k):
        arrived = GOT.at[k, pl.ds(0, devices - 1)]
        pltpu.make_async_copy(arrived, arrived, all_recv.at[k]).wait()

    def collect(k):
        wait_row(k)
        value = (GOT[k, 0], jnp.zeros((2, 128), jnp.float32))
        for d in range(1, devices):
            s, e = two_sum(value[0], GOT[k, d])
            value = (s, value[1] + e)
        high = jnp.broadcast_to(value[0][0:1], (8, 128))
        low = jnp.broadcast_to(value[1][0:1] + value[0][1:2], (8, 128))
        return quick(high, low)

    for copy in loads[:4]:
        copy.wait()
    pl.semaphore_wait(barrier, devices - 1)
    send(0, "v", 0)
    scale_diag(GHOST, deep)
    scale_diag(GHOST + planes - deep, deep)
    for which, kind, plane in order[1:]:
        if which == 0:
            send(0, kind, plane)
    for copy in loads[4:]:
        copy.wait()
    scale_diag(GHOST + deep, planes - 2 * deep)

    n = STEPS
    for index, (base, steps) in enumerate(zip(BASES, BLOCKS)):
        final = index + 1 == len(BLOCKS)
        after = 0 if final else BLOCKS[index + 1]
        rows_from = base + 1 if index else 0
        for which, kind, plane in order:
            if index and which == index and kind == "d":
                send(index, kind, plane)
        inner(base, steps)
        for plane in range(steps, after):
            send(index + 1, "v", plane)
        if index:
            outer_products(BASES[index - 1] + 1 if index > 1 else 0, base, BLOCKS[index - 1])
        inner_products(rows_from, n - 1 if final else base + steps, steps - 1 if final else steps)
        if final:
            inner_products(n, n, steps)
        for g in range(1, steps + 1):
            receive(index, "v", g - 1)
            if g > 1 and ("d", g - 2) in numbers:
                which = order[numbers[("d", g - 2)]][0]
                if which == index or (index > 0 and which == index - 1 and g - 1 >= BLOCKS[index - 1]):
                    receive(which, "d", g - 2)
            wave(base, steps, g)
            if index == 0 and steps - g < after:
                send(index + 1, "v", steps - g)
            if final:
                if g < steps:
                    near = steps - 1 - g
                    products(
                        base + 1,
                        n - 1,
                        (GHOST + near, GHOST + planes - 1 - near),
                        planes // 2 - steps + g,
                    )
                near = steps - g
                products(n, n, (GHOST + near, GHOST + planes - 1 - near), planes // 2 - steps + g - 1)
                if g == steps - 1:
                    where = {
                        (i, j): sorted({n * i + j, n * j + i}) for i, j in pairs if j < n
                    }
                    share(0, reduce(where, n * n))
        if index:
            for plane in range(min(steps, after)):
                send(index + 1, "v", plane)
    share(1, reduce({(i, n): [i] for i in range(n)}, n))
    wait_sent()
    wait_shared()

    table_load.wait()
    sub = lax.broadcasted_iota(jnp.int32, (8, 128), 0)
    got = collect(0)
    parts = []
    for h in range(2):
        top, bottom = zero, zero
        for i in range(n):
            moved = got[h] if i == 0 else pltpu.roll(got[h], 128 - n * i, 1)
            if i < 8:
                top = jnp.where(sub == i, moved, top)
            else:
                bottom = jnp.where(sub == i - 8, moved, bottom)
        both = jnp.concatenate([top, bottom], axis=0)
        wide = lax.broadcasted_iota(jnp.int32, (16, 128), 1)
        parts.append(jnp.where(wide < n, both, TAB[h, 0:16, :]))
    M = tuple(parts)
    row = lax.broadcasted_iota(jnp.int32, (16, 128), 0)
    for k in range(n):
        column = tuple(jnp.broadcast_to(m[:, k : k + 1], (16, 128)) for m in M)
        pivot = tuple(jnp.broadcast_to(c[k : k + 1, :], (16, 128)) for c in column)
        scaled = mul2(tuple(jnp.broadcast_to(m[k : k + 1, :], (16, 128)) for m in M), inverse2(pivot))
        rest = add2(M, neg2(mul2(column, scaled)))
        M = tuple(jnp.where(row == k, s, m) for s, m in zip(scaled, rest))
    got = collect(1)
    wide = lax.broadcasted_iota(jnp.int32, (16, 128), 1)
    H = tuple(
        jnp.broadcast_to(
            jnp.sum(
                jnp.where(wide == row, jnp.concatenate([v, v], axis=0), 0.0), axis=1, keepdims=True
            ),
            (16, 128),
        )
        for v in got
    )
    H = tuple(jnp.where(row < n, v, 0.0) for v in H)
    M = tuple(jnp.where(row < n, m, 0.0) for m in M)
    terms = mul2(M, H)
    terms = sublanes2(add2(tuple(t[0:8] for t in terms), tuple(t[8:16] for t in terms)))
    terms = add2(terms, (TAB[0, 16:24, :], TAB[1, 16:24, :]))
    value = tuple(
        jnp.broadcast_to(t[:, SHIFT + 2 * n + 1 : SHIFT + 2 * n + 2], (8, 128)) for t in terms
    )
    terms = mul2(terms, inverse2(value))
    factor = terms[0]
    fx = [jnp.broadcast_to(factor[:, SHIFT + i : SHIFT + i + 1], (8, 128)) for i in range(n)]
    fr = [
        jnp.broadcast_to(factor[:, SHIFT + n + i : SHIFT + n + i + 1], (8, 128))
        for i in range(n + 1)
    ]

    def one(i, _):
        plane = GHOST + i
        for c in range(chunks):
            at = pl.ds(PAD + 8 * c, 8)
            v = [V[k, plane, at, :] for k in range(n + 1)]
            x_ref[i, 8 * c : 8 * c + 8, :] = functools.reduce(jnp.add, [f * u for f, u in zip(fx, v)])
            r_ref[i, 8 * c : 8 * c + 8, :] = functools.reduce(jnp.add, [f * u for f, u in zip(fr, v)])
        return 0

    lax.fori_loop(0, planes, one, 0)


def store_kernel(x_ref, r_ref, x_out, r_out, sem):
    group = x_ref.shape[0] // 4
    copies = []
    for q in range(4):
        for k, (source, target) in enumerate(((x_ref, x_out), (r_ref, r_out))):
            at = pl.ds(group * q, group)
            copies.append(pltpu.make_async_copy(source.at[at], target.at[at], sem.at[k, q]))
            copies[-1].start()
    for copy in copies:
        copy.wait()


def local(right_side, diagonal):
    planes, rows, lanes = right_side.shape
    devices = lax.axis_size("slab")
    tall = planes + 2 * GHOST
    f32 = jnp.float32
    out = jax.ShapeDtypeStruct(right_side.shape, f32)
    held = pltpu.VMEM(right_side.shape, f32)
    dma = pltpu.SemaphoreType.DMA
    results = pl.pallas_call(
        functools.partial(kernel, devices),
        out_shape=(held, held),
        in_specs=[pl.BlockSpec(memory_space=pltpu.HBM)] * 3,
        out_specs=(pl.BlockSpec(memory_space=pltpu.VMEM),) * 2,
        scratch_shapes=[
            pltpu.VMEM((STEPS + 1, tall, rows + 2 * PAD, lanes), f32),
            pltpu.VMEM((tall, rows + 2 * PAD, lanes), f32),
            pltpu.VMEM(((STEPS + 1) * (STEPS + 2) // 2, SLOTS, 8, 128), f32),
            pltpu.VMEM((2, 1024, 128), f32),
            pltpu.VMEM((2, 128, 128), f32),
            pltpu.VMEM((2, 2, 128), f32),
            pltpu.VMEM((2, devices, 2, 128), f32),
            pltpu.VMEM((2, 24, 128), f32),
            dma((7,)),
            dma((2,)),
            dma((2, MESSAGES)),
            dma((2,)),
            dma((2,)),
        ],
        compiler_params=pltpu.CompilerParams(
            collective_id=0, has_side_effects=True, vmem_limit_bytes=40 * 2**20
        ),
        name="cg",
    )(
        *(
            pltpu.with_memory_space_constraint(a, pltpu.HBM)
            for a in (right_side, diagonal, jnp.asarray(tables()))
        )
    )
    return pl.pallas_call(
        store_kernel,
        out_shape=(out, out),
        in_specs=[pl.BlockSpec(memory_space=pltpu.VMEM)] * 2,
        out_specs=(pl.BlockSpec(memory_space=pltpu.HBM),) * 2,
        scratch_shapes=[dma((2, 4))],
        name="store",
    )(*(pltpu.with_memory_space_constraint(a, pltpu.VMEM) for a in results))


def solution(mesh):
    placed = (P("slab", "sys", None), P("slab", "sys", None))
    return jax.shard_map(
        local,
        mesh=mesh,
        in_specs=placed,
        out_specs=placed,
        check_vma=False,
    )
```

```python
import functools

import jax
import jax.numpy as jnp
import numpy as np
from jax import lax
from jax.experimental import pallas as pl
from jax.experimental.pallas import tpu as pltpu
from jax.sharding import PartitionSpec as P

MID = 7.125
HALF = 6.875
BLOCKS = (3, 3, 4)
STEPS = sum(BLOCKS)
BASES = tuple(int(b) for b in np.cumsum((0,) + BLOCKS[:-1]))
GHOST = max(BLOCKS)
MESSAGES = STEPS + GHOST - 1
PAD = 8
SLOTS = 8
SHIFT = 32
MESH = pl.DeviceIdType.MESH


def tables():
    n = STEPS
    apply = np.zeros((n + 1, n))
    at_zero = np.zeros(n + 1)
    at_zero[0] = 1.0
    for base, steps in zip(BASES, BLOCKS):
        for j in range(steps):
            i = base + j
            apply[i, i] = MID
            if j == 0:
                apply[i + 1, i] = HALF
                at_zero[i + 1] = -MID / HALF * at_zero[i]
            else:
                apply[i + 1, i] = apply[i - 1, i] = HALF / 2
                at_zero[i + 1] = -2 * MID / HALF * at_zero[i] - at_zero[i - 1]
    divide = np.zeros((n, n + 1))
    divide[:, 1:] = -np.linalg.inv(apply[1:])
    maps = np.concatenate([divide, np.eye(n + 1), at_zero[None]]).T
    sides = np.zeros((24, 128))
    sides[:n, SHIFT : SHIFT + maps.shape[1]] = -maps[:n]
    sides[16:, SHIFT : SHIFT + maps.shape[1]] = maps[n]
    high = sides.astype(np.float32)
    return np.stack([high, (sides - high).astype(np.float32)])


def two_sum(a, b):
    s = a + b
    t = s - a
    return s, (a - (s - t)) + (b - t)


def quick(a, b):
    s = a + b
    return s, b - (s - a)


def halves(a):
    c = a * 4097.0
    h = c - (c - a)
    return h, a - h


def add2(a, b):
    s, e = two_sum(a[0], b[0])
    return quick(s, e + (a[1] + b[1]))


def mul2(a, b):
    p = a[0] * b[0]
    ah, al = halves(a[0])
    bh, bl = halves(b[0])
    e = ((ah * bh - p) + (ah * bl + al * bh)) + al * bl
    return quick(p, e + (a[0] * b[1] + a[1] * b[0]))


def neg2(a):
    return (-a[0], -a[1])


def inverse2(a):
    y = 1.0 / a[0]
    zero = jnp.zeros_like(y)
    p, e = mul2(a, (y, zero))
    return quick(y, y * ((1.0 - p) - e))


def tree2(parts):
    while len(parts) > 1:
        parts = [add2(parts[i], parts[i + 1]) for i in range(0, len(parts) - 1, 2)] + (
            [parts[-1]] if len(parts) % 2 else []
        )
    return parts[0]


def sublanes2(a):
    for shift in (4, 2, 1):
        a = add2(a, tuple(pltpu.roll(v, shift, 0) for v in a))
    return a


def kernel(
    devices,
    right_ref,
    diag_ref,
    table_ref,
    V,
    COEF,
    D,
    ACC,
    RED,
    PACK,
    SEND,
    GOT,
    TAB,
    load_sem,
    send_sem,
    recv_sem,
    all_send,
    all_recv,
):
    planes, rows = right_ref.shape[0], right_ref.shape[1]
    chunks = rows // 8
    me = lax.axis_index("slab")
    below = lax.rem(me + devices - 1, devices)
    above = lax.rem(me + 1, devices)
    has_below = me > 0
    has_above = me < devices - 1
    body = pl.ds(PAD, rows)
    deep = GHOST

    def load(ref, at, first, count, sem):
        return pltpu.make_async_copy(
            ref.at[pl.ds(first, count)], at.at[pl.ds(GHOST + first, count), body], load_sem.at[sem]
        )

    loads = []
    for sem, (ref, at) in enumerate(((right_ref, V.at[0]), (diag_ref, D))):
        loads.append(load(ref, at, 0, deep, 3 * sem))
        loads.append(load(ref, at, planes - deep, deep, 3 * sem + 1))
    for sem, (ref, at) in enumerate(((right_ref, V.at[0]), (diag_ref, D))):
        loads.append(load(ref, at, deep, planes - 2 * deep, 3 * sem + 2))
    table_load = pltpu.make_async_copy(table_ref, TAB, load_sem.at[6])
    for copy in loads:
        copy.start()
    table_load.start()

    barrier = pltpu.get_barrier_semaphore()
    for o in range(1, devices):
        pl.semaphore_signal(
            barrier, inc=1, device_id={"slab": lax.rem(me + o, devices)}, device_id_type=MESH
        )

    zero = jnp.zeros((8, 128), jnp.float32)

    def clear(i, _):
        for k in range(STEPS):
            V[k, i, 0:8, :] = zero
            V[k, i, PAD + rows : PAD + rows + 8, :] = zero
        return 0

    lax.fori_loop(0, planes + 2 * GHOST, clear, 0)

    def clear_ghost(first):
        for base in BASES:
            for i in range(GHOST):
                for c in range(chunks):
                    V[base, first + i, PAD + 8 * c : PAD + 8 * c + 8, :] = zero

    @pl.when(jnp.logical_not(has_below))
    def _():
        clear_ghost(0)

    @pl.when(jnp.logical_not(has_above))
    def _():
        clear_ghost(GHOST + planes)

    def message(array, plane, up, t):
        if up:
            source, target = GHOST + planes - 1 - plane, GHOST - 1 - plane
        else:
            source, target = GHOST + plane, GHOST + planes + plane
        return pltpu.make_async_remote_copy(
            src_ref=array.at[source, body],
            dst_ref=array.at[target, body],
            send_sem=send_sem.at[int(up)],
            recv_sem=recv_sem.at[int(up), t],
            device_id={"slab": above if up else below},
            device_id_type=MESH,
        )

    numbers = {}
    order = []
    diag_sent = 0
    for index, (base, steps) in enumerate(zip(BASES, BLOCKS)):
        for plane in range(steps):
            order.append((index, "v", plane))
            if index == 0 and plane < steps - 1:
                order.append((index, "d", plane))
        upto = steps - 1 if index + 1 == len(BLOCKS) else max(BLOCKS[: index + 2]) - 1
        for plane in range(max(diag_sent, BLOCKS[0] - 1), upto):
            order.append((index, "d", plane))
        diag_sent = max(upto, diag_sent, BLOCKS[0] - 1)
    for t, (index, kind, plane) in enumerate(order):
        numbers[(kind, plane) if kind == "d" else (kind, index, plane)] = t

    def of(index, kind, plane, up):
        t = numbers[(kind, plane) if kind == "d" else (kind, index, plane)]
        return message(D if kind == "d" else V.at[BASES[index]], plane, up, t)

    def send(index, kind, plane):
        @pl.when(has_below)
        def _():
            of(index, kind, plane, False).start()

        @pl.when(has_above)
        def _():
            of(index, kind, plane, True).start()

    def wait_sent():
        for up, there in ((False, has_below), (True, has_above)):

            @pl.when(there)
            def _(up=up):
                sent = D.at[pl.ds(0, len(order)), body]
                pltpu.make_async_copy(sent, sent, send_sem.at[int(up)]).wait()

    def receive(index, kind, plane):
        @pl.when(has_below)
        def _():
            of(index, kind, plane, True).wait_recv()

        @pl.when(has_above)
        def _():
            of(index, kind, plane, False).wait_recv()

    lane = lax.broadcasted_iota(jnp.int32, (8, 128), 1)
    leftmost, rightmost = lane == 0, lane == 127
    scale = np.float32(2.0 / HALF)

    def scale_diag(first, count):
        def one(i, _):
            for c in range(chunks):
                at = pl.ds(PAD + 8 * c, 8)
                D[first + i, at, :] = (D[first + i, at, :] + np.float32(6.0 - MID)) * scale
            return 0

        lax.fori_loop(0, count, one, 0)

    def step(source, target, before, plane, keep=None):
        for c in range(chunks):
            at = pl.ds(PAD + 8 * c, 8)
            v = V[source, plane, at, :]
            sides = (V[source, plane - 1, at, :] + V[source, plane + 1, at, :]) + (
                V[source, plane, pl.ds(PAD + 8 * c - 1, 8), :]
                + V[source, plane, pl.ds(PAD + 8 * c + 1, 8), :]
            )
            sides = sides + (
                jnp.where(leftmost, 0.0, pltpu.roll(v, 1, 1))
                + jnp.where(rightmost, 0.0, pltpu.roll(v, 127, 1))
            )
            new = D[plane, at, :] * v - scale * sides
            new = 0.5 * new if before is None else new - V[before, plane, at, :]
            V[target, plane, at, :] = new if keep is None else jnp.where(keep, new, 0.0)

    def inner(base, steps, near):
        for j in range(1, steps + 1):
            before = None if j == 1 else base + j - 2

            def pair(i, _, j=j, before=before):
                first = GHOST + near + j + 2 * i
                step(base + j - 1, base + j, before, first)
                step(base + j - 1, base + j, before, first + 1)
                return 0

            lax.fori_loop(0, planes // 2 - near - j, pair, 0)

    def inner_rest(base, steps, near):
        for j in range(1, steps + 1):
            before = None if j == 1 else base + j - 2
            for i in range(j, j + near):
                step(base + j - 1, base + j, before, GHOST + i)
                step(base + j - 1, base + j, before, GHOST + planes - 1 - i)

    def wave(base, steps, g):
        low, high = GHOST - g, GHOST + planes - 1 + g

        def one(j, before):
            keep_low, keep_high = (None, None) if j >= g else (has_below, has_above)
            step(base + j - 1, base + j, before, low + j, keep_low)
            step(base + j - 1, base + j, before, high - j, keep_high)

        for j in range(1, steps + 1):
            one(j, None if j == 1 else base + j - 2)

    pairs = [(i, j) for j in range(STEPS + 1) for i in range(j + 1)]
    place = {pair: i for i, pair in enumerate(pairs)}

    def products(first, last, two, slot):
        mine = [p for p in pairs if first <= p[1] <= last and p != (STEPS, STEPS)]

        def add(plane):
            def some(c, acc):
                acc = list(acc)
                for u in range(4):
                    at = pl.ds(pl.multiple_of(PAD + 32 * c + 8 * u, 8), 8)
                    v = [V[k, plane, at, :] for k in range(last + 1)]
                    for a, (i, j) in enumerate(mine):
                        acc[a] = acc[a] + v[i] * v[j]
                return tuple(acc)

            return some

        acc = tuple(zero for _ in mine)
        for plane in two:
            acc = lax.fori_loop(0, chunks // 4, add(plane), acc)
        for value, pair in zip(acc, mine):
            ACC[place[pair], slot] = value

    def middle_products(first, last, near):
        def one(slot, _):
            at = GHOST + near + 2 * slot
            products(first, last, (at, at + 1), slot)
            return 0

        lax.fori_loop(0, planes // 2 - near, one, 0)

    def side_products(first, last, start, stop):
        def one(i, _):
            products(first, last, (GHOST + i, GHOST + planes - 1 - i), planes // 2 - 1 - i)
            return 0

        lax.fori_loop(start, stop, one, 0)

    def reduce(where, count):
        for pair, lanes in where.items():
            value = (ACC[place[pair], 0], zero)
            for slot in range(1, SLOTS):
                s, e = two_sum(value[0], ACC[place[pair], slot])
                value = (s, value[1] + e)
            for n in lanes:
                RED[0, 8 * n : 8 * n + 8, :] = value[0]
                RED[1, 8 * n : 8 * n + 8, :] = value[1]
        for q in range(16):
            if 8 * q >= count:
                PACK[0, 8 * q : 8 * q + 8, :] = zero
                PACK[1, 8 * q : 8 * q + 8, :] = zero
                continue
            total = tree2(
                [
                    tuple(RED[h, pl.ds(64 * q + s, 8, stride=8), :] for h in range(2))
                    for s in range(8)
                ]
            )
            PACK[0, 8 * q : 8 * q + 8, :] = total[0]
            PACK[1, 8 * q : 8 * q + 8, :] = total[1]
        high, low = jnp.transpose(PACK[0]), jnp.transpose(PACK[1])
        total = sublanes2(
            tree2([(high[8 * q : 8 * q + 8], low[8 * q : 8 * q + 8]) for q in range(16)])
        )
        return total

    def spread(k, o):
        return pltpu.make_async_remote_copy(
            src_ref=SEND.at[k],
            dst_ref=GOT.at[k, me],
            send_sem=all_send.at[k],
            recv_sem=all_recv.at[k],
            device_id={"slab": lax.rem(me + o, devices)},
            device_id_type=MESH,
        )

    def share(k, total):
        SEND[k, 0:1, :] = total[0][0:1]
        SEND[k, 1:2, :] = total[1][0:1]
        GOT[k, me, 0:1, :] = total[0][0:1]
        GOT[k, me, 1:2, :] = total[1][0:1]
        for o in range(1, devices):
            spread(k, o).start()

    def wait_shared():
        for k in range(2):
            sent = GOT.at[k, pl.ds(0, devices - 1)]
            pltpu.make_async_copy(sent, sent, all_send.at[k]).wait()

    def wait_row(k):
        arrived = GOT.at[k, pl.ds(0, devices - 1)]
        pltpu.make_async_copy(arrived, arrived, all_recv.at[k]).wait()

    def collect(k):
        wait_row(k)
        value = (GOT[k, 0], jnp.zeros((2, 128), jnp.float32))
        for d in range(1, devices):
            s, e = two_sum(value[0], GOT[k, d])
            value = (s, value[1] + e)
        high = jnp.broadcast_to(value[0][0:1], (8, 128))
        low = jnp.broadcast_to(value[1][0:1] + value[0][1:2], (8, 128))
        return quick(high, low)

    for copy in loads[:4]:
        copy.wait()
    pl.semaphore_wait(barrier, devices - 1)
    send(0, "v", 0)
    scale_diag(GHOST, deep)
    scale_diag(GHOST + planes - deep, deep)
    for which, kind, plane in order[1:]:
        if which == 0:
            send(0, kind, plane)
    for copy in loads[4:]:
        copy.wait()
    scale_diag(GHOST + deep, planes - 2 * deep)

    n = STEPS

    def begin(index):
        base, steps, near = BASES[index], BLOCKS[index], BLOCKS[index - 1] if index else 0
        final = index + 1 == len(BLOCKS)
        inner(base, steps, near)
        last = n - 1 if final else base + steps
        middle_products(base + 1 if index else 0, last, near + steps - final)
        if final:
            middle_products(n, n, near + steps)

    begin(0)
    for index, (base, steps) in enumerate(zip(BASES, BLOCKS)):
        final = index + 1 == len(BLOCKS)
        after = 0 if final else BLOCKS[index + 1]
        if index:
            near = BLOCKS[index - 1]
            for which, kind, plane in order:
                if which == index and kind == "d":
                    send(index, kind, plane)
            inner_rest(base, steps, near)
            for plane in range(steps, after):
                send(index + 1, "v", plane)
            side_products(BASES[index - 1] + 1 if index > 1 else 0, base, 0, near)
            if final:
                side_products(base + 1, n - 1, steps - 1, steps - 1 + near)
                side_products(n, n, steps, steps + near)
            else:
                side_products(base + 1, base + steps, steps, steps + near)
                begin(index + 1)
        for g in range(1, steps + 1):
            receive(index, "v", g - 1)
            if g > 1 and ("d", g - 2) in numbers:
                which = order[numbers[("d", g - 2)]][0]
                if which == index or (index > 0 and which == index - 1 and g - 1 >= BLOCKS[index - 1]):
                    receive(which, "d", g - 2)
            wave(base, steps, g)
            if index == 0:
                if steps - g < after:
                    send(1, "v", steps - g)
                if g == 1:
                    for plane in range(steps, after):
                        send(1, "v", plane)
                    begin(1)
            if final:
                if g < steps:
                    near = steps - 1 - g
                    products(
                        base + 1,
                        n - 1,
                        (GHOST + near, GHOST + planes - 1 - near),
                        planes // 2 - 1 - near,
                    )
                near = steps - g
                products(n, n, (GHOST + near, GHOST + planes - 1 - near), planes // 2 - 1 - near)
                if g == steps - 1:
                    where = {
                        (i, j): sorted({n * i + j, n * j + i}) for i, j in pairs if j < n
                    }
                    share(0, reduce(where, n * n))
        if index:
            for plane in range(min(steps, after)):
                send(index + 1, "v", plane)
    share(1, reduce({(i, n): [i] for i in range(n)}, n))
    wait_sent()
    wait_shared()

    table_load.wait()
    sub = lax.broadcasted_iota(jnp.int32, (8, 128), 0)
    got = collect(0)
    parts = []
    for h in range(2):
        top, bottom = zero, zero
        for i in range(n):
            moved = got[h] if i == 0 else pltpu.roll(got[h], 128 - n * i, 1)
            if i < 8:
                top = jnp.where(sub == i, moved, top)
            else:
                bottom = jnp.where(sub == i - 8, moved, bottom)
        both = jnp.concatenate([top, bottom], axis=0)
        wide = lax.broadcasted_iota(jnp.int32, (16, 128), 1)
        parts.append(jnp.where(wide < n, both, TAB[h, 0:16, :]))
    M = tuple(parts)
    row = lax.broadcasted_iota(jnp.int32, (16, 128), 0)
    for k in range(n):
        column = tuple(jnp.broadcast_to(m[:, k : k + 1], (16, 128)) for m in M)
        pivot = tuple(jnp.broadcast_to(c[k : k + 1, :], (16, 128)) for c in column)
        scaled = mul2(tuple(jnp.broadcast_to(m[k : k + 1, :], (16, 128)) for m in M), inverse2(pivot))
        rest = add2(M, neg2(mul2(column, scaled)))
        M = tuple(jnp.where(row == k, s, m) for s, m in zip(scaled, rest))
    got = collect(1)
    wide = lax.broadcasted_iota(jnp.int32, (16, 128), 1)
    H = tuple(
        jnp.broadcast_to(
            jnp.sum(
                jnp.where(wide == row, jnp.concatenate([v, v], axis=0), 0.0), axis=1, keepdims=True
            ),
            (16, 128),
        )
        for v in got
    )
    H = tuple(jnp.where(row < n, v, 0.0) for v in H)
    M = tuple(jnp.where(row < n, m, 0.0) for m in M)
    terms = mul2(M, H)
    terms = sublanes2(add2(tuple(t[0:8] for t in terms), tuple(t[8:16] for t in terms)))
    terms = add2(terms, (TAB[0, 16:24, :], TAB[1, 16:24, :]))
    value = tuple(
        jnp.broadcast_to(t[:, SHIFT + 2 * n + 1 : SHIFT + 2 * n + 2], (8, 128)) for t in terms
    )
    terms = mul2(terms, inverse2(value))
    factor = terms[0]
    for i in range(2 * n + 1):
        COEF[i] = jnp.broadcast_to(factor[:, SHIFT + i : SHIFT + i + 1], (8, 128))


def combine_kernel(V, COEF, x_out, r_out, X, R, sem):
    planes, rows = X.shape[0], X.shape[1]
    n = STEPS
    fx = [COEF[i] for i in range(n)]
    fr = [COEF[n + i] for i in range(n + 1)]

    def one(i, _):
        for c in range(rows // 8):
            at = pl.ds(8 * c, 8)
            v = [V[k, GHOST + i, pl.ds(PAD + 8 * c, 8), :] for k in range(n + 1)]
            X[i, at, :] = functools.reduce(jnp.add, [f * u for f, u in zip(fx, v)])
            R[i, at, :] = functools.reduce(jnp.add, [f * u for f, u in zip(fr, v)])
        return 0

    copies = []
    group = 2
    for q in range(planes // group):
        lax.fori_loop(group * q, group * q + group, one, 0)
        at = pl.ds(group * q, group)
        for k, (source, target) in enumerate(((X, x_out), (R, r_out))):
            copies.append(pltpu.make_async_copy(source.at[at], target.at[at], sem.at[k, q]))
            copies[-1].start()
    for copy in copies:
        copy.wait()


def local(right_side, diagonal):
    planes, rows, lanes = right_side.shape
    devices = lax.axis_size("slab")
    tall = planes + 2 * GHOST
    f32 = jnp.float32
    out = jax.ShapeDtypeStruct(right_side.shape, f32)
    held = (
        pltpu.VMEM((STEPS + 1, tall, rows + 2 * PAD, lanes), f32),
        pltpu.VMEM((2 * STEPS + 1, 8, 128), f32),
    )
    dma = pltpu.SemaphoreType.DMA
    results = pl.pallas_call(
        functools.partial(kernel, devices),
        out_shape=held,
        in_specs=[pl.BlockSpec(memory_space=pltpu.HBM)] * 3,
        out_specs=(pl.BlockSpec(memory_space=pltpu.VMEM),) * 2,
        scratch_shapes=[
            pltpu.VMEM((tall, rows + 2 * PAD, lanes), f32),
            pltpu.VMEM(((STEPS + 1) * (STEPS + 2) // 2, SLOTS, 8, 128), f32),
            pltpu.VMEM((2, 1024, 128), f32),
            pltpu.VMEM((2, 128, 128), f32),
            pltpu.VMEM((2, 2, 128), f32),
            pltpu.VMEM((2, devices, 2, 128), f32),
            pltpu.VMEM((2, 24, 128), f32),
            dma((7,)),
            dma((2,)),
            dma((2, MESSAGES)),
            dma((2,)),
            dma((2,)),
        ],
        compiler_params=pltpu.CompilerParams(
            collective_id=0, has_side_effects=True, vmem_limit_bytes=16 * 2**20
        ),
        name="cg",
    )(
        *(
            pltpu.with_memory_space_constraint(a, pltpu.HBM)
            for a in (right_side, diagonal, jnp.asarray(tables()))
        )
    )
    return pl.pallas_call(
        combine_kernel,
        out_shape=(out, out),
        in_specs=[pl.BlockSpec(memory_space=pltpu.VMEM)] * 2,
        out_specs=(pl.BlockSpec(memory_space=pltpu.HBM),) * 2,
        scratch_shapes=[
            pltpu.VMEM(right_side.shape, f32),
            pltpu.VMEM(right_side.shape, f32),
            dma((2, planes // 2)),
        ],
        compiler_params=pltpu.CompilerParams(vmem_limit_bytes=8 * 2**20),
        name="combine",
    )(*(pltpu.with_memory_space_constraint(a, pltpu.VMEM) for a in results))


def solution(mesh):
    placed = (P("slab", "sys", None), P("slab", "sys", None))
    return jax.shard_map(
        local,
        mesh=mesh,
        in_specs=placed,
        out_specs=placed,
        check_vma=False,
    )
```

```python
import functools

import jax
import jax.numpy as jnp
import numpy as np
from jax import lax
from jax.experimental import pallas as pl
from jax.experimental.pallas import tpu as pltpu
from jax.sharding import PartitionSpec as P

MID = 7.125
HALF = 6.875
BLOCKS = (3, 3, 4)
STEPS = sum(BLOCKS)
BASES = tuple(int(b) for b in np.cumsum((0,) + BLOCKS[:-1]))
GHOST = max(BLOCKS)
MESSAGES = STEPS + GHOST - 1
PAD = 8
SLOTS = 8
SHIFT = 32
WHOLE = 64
LATE = 16
MESH = pl.DeviceIdType.MESH


def tables():
    n = STEPS
    apply = np.zeros((n + 1, n))
    at_zero = np.zeros(n + 1)
    at_zero[0] = 1.0
    for base, steps in zip(BASES, BLOCKS):
        for j in range(steps):
            i = base + j
            apply[i, i] = MID
            if j == 0:
                apply[i + 1, i] = HALF
                at_zero[i + 1] = -MID / HALF * at_zero[i]
            else:
                apply[i + 1, i] = apply[i - 1, i] = HALF / 2
                at_zero[i + 1] = -2 * MID / HALF * at_zero[i] - at_zero[i - 1]
    divide = np.zeros((n, n + 1))
    divide[:, 1:] = -np.linalg.inv(apply[1:])
    maps = np.concatenate([divide, np.eye(n + 1), at_zero[None]]).T
    sides = np.zeros((32, 128))
    wide = slice(SHIFT, SHIFT + maps.shape[1])
    sides[: n - 1, wide] = maps[: n - 1]
    sides[: n - 1, WHOLE : WHOLE + n - 1] = np.eye(n - 1)
    sides[16:24, wide] = maps[n - 1]
    sides[24:, wide] = maps[n]
    high = sides.astype(np.float32)
    return np.stack([high, (sides - high).astype(np.float32)])


def two_sum(a, b):
    s = a + b
    t = s - a
    return s, (a - (s - t)) + (b - t)


def quick(a, b):
    s = a + b
    return s, b - (s - a)


def halves(a):
    c = a * 4097.0
    h = c - (c - a)
    return h, a - h


def add2(a, b):
    s, e = two_sum(a[0], b[0])
    return quick(s, e + (a[1] + b[1]))


def mul2(a, b):
    p = a[0] * b[0]
    ah, al = halves(a[0])
    bh, bl = halves(b[0])
    e = ((ah * bh - p) + (ah * bl + al * bh)) + al * bl
    return quick(p, e + (a[0] * b[1] + a[1] * b[0]))


def neg2(a):
    return (-a[0], -a[1])


def inverse2(a):
    y = 1.0 / a[0]
    zero = jnp.zeros_like(y)
    p, e = mul2(a, (y, zero))
    return quick(y, y * ((1.0 - p) - e))


def tree2(parts):
    while len(parts) > 1:
        parts = [add2(parts[i], parts[i + 1]) for i in range(0, len(parts) - 1, 2)] + (
            [parts[-1]] if len(parts) % 2 else []
        )
    return parts[0]


def sublanes2(a):
    for shift in (4, 2, 1):
        a = add2(a, tuple(pltpu.roll(v, shift, 0) for v in a))
    return a


def kernel(
    devices,
    right_ref,
    diag_ref,
    table_ref,
    V,
    COEF,
    D,
    ACC,
    RED,
    PACK,
    SEND,
    GOT,
    TAB,
    load_sem,
    send_sem,
    recv_sem,
    all_send,
    all_recv,
):
    planes, rows = right_ref.shape[0], right_ref.shape[1]
    chunks = rows // 8
    me = lax.axis_index("slab")
    below = lax.rem(me + devices - 1, devices)
    above = lax.rem(me + 1, devices)
    has_below = me > 0
    has_above = me < devices - 1
    body = pl.ds(PAD, rows)
    deep = GHOST

    def load(ref, at, first, count, sem):
        return pltpu.make_async_copy(
            ref.at[pl.ds(first, count)], at.at[pl.ds(GHOST + first, count), body], load_sem.at[sem]
        )

    loads = []
    for sem, (ref, at) in enumerate(((right_ref, V.at[0]), (diag_ref, D))):
        loads.append(load(ref, at, 0, deep, 3 * sem))
        loads.append(load(ref, at, planes - deep, deep, 3 * sem + 1))
    for sem, (ref, at) in enumerate(((right_ref, V.at[0]), (diag_ref, D))):
        loads.append(load(ref, at, deep, planes - 2 * deep, 3 * sem + 2))
    table_load = pltpu.make_async_copy(table_ref, TAB, load_sem.at[6])
    for copy in loads:
        copy.start()
    table_load.start()

    barrier = pltpu.get_barrier_semaphore()
    for o in range(1, devices):
        pl.semaphore_signal(
            barrier, inc=1, device_id={"slab": lax.rem(me + o, devices)}, device_id_type=MESH
        )

    zero = jnp.zeros((8, 128), jnp.float32)

    def clear(i, _):
        for k in range(STEPS):
            V[k, i, 0:8, :] = zero
            V[k, i, PAD + rows : PAD + rows + 8, :] = zero
        return 0

    lax.fori_loop(0, planes + 2 * GHOST, clear, 0)

    def clear_ghost(first):
        for base in BASES:
            for i in range(GHOST):
                for c in range(chunks):
                    V[base, first + i, PAD + 8 * c : PAD + 8 * c + 8, :] = zero

    @pl.when(jnp.logical_not(has_below))
    def _():
        clear_ghost(0)

    @pl.when(jnp.logical_not(has_above))
    def _():
        clear_ghost(GHOST + planes)

    def message(array, plane, up, t):
        if up:
            source, target = GHOST + planes - 1 - plane, GHOST - 1 - plane
        else:
            source, target = GHOST + plane, GHOST + planes + plane
        return pltpu.make_async_remote_copy(
            src_ref=array.at[source, body],
            dst_ref=array.at[target, body],
            send_sem=send_sem.at[int(up)],
            recv_sem=recv_sem.at[int(up), t],
            device_id={"slab": above if up else below},
            device_id_type=MESH,
        )

    numbers = {}
    order = []
    diag_sent = 0
    for index, (base, steps) in enumerate(zip(BASES, BLOCKS)):
        for plane in range(steps):
            order.append((index, "v", plane))
            if index == 0 and plane < steps - 1:
                order.append((index, "d", plane))
        upto = steps - 1 if index + 1 == len(BLOCKS) else max(BLOCKS[: index + 2]) - 1
        for plane in range(max(diag_sent, BLOCKS[0] - 1), upto):
            order.append((index, "d", plane))
        diag_sent = max(upto, diag_sent, BLOCKS[0] - 1)
    for t, (index, kind, plane) in enumerate(order):
        numbers[(kind, plane) if kind == "d" else (kind, index, plane)] = t

    def of(index, kind, plane, up):
        t = numbers[(kind, plane) if kind == "d" else (kind, index, plane)]
        return message(D if kind == "d" else V.at[BASES[index]], plane, up, t)

    def send(index, kind, plane):
        @pl.when(has_below)
        def _():
            of(index, kind, plane, False).start()

        @pl.when(has_above)
        def _():
            of(index, kind, plane, True).start()

    def wait_sent():
        for up, there in ((False, has_below), (True, has_above)):

            @pl.when(there)
            def _(up=up):
                sent = D.at[pl.ds(0, len(order)), body]
                pltpu.make_async_copy(sent, sent, send_sem.at[int(up)]).wait()

    def receive(index, kind, plane):
        @pl.when(has_below)
        def _():
            of(index, kind, plane, True).wait_recv()

        @pl.when(has_above)
        def _():
            of(index, kind, plane, False).wait_recv()

    lane = lax.broadcasted_iota(jnp.int32, (8, 128), 1)
    leftmost, rightmost = lane == 0, lane == 127
    scale = np.float32(2.0 / HALF)

    def scale_diag(first, count):
        def one(i, _):
            for c in range(chunks):
                at = pl.ds(PAD + 8 * c, 8)
                D[first + i, at, :] = (D[first + i, at, :] + np.float32(6.0 - MID)) * scale
            return 0

        lax.fori_loop(0, count, one, 0)

    def step(source, target, before, plane, keep=None):
        for c in range(chunks):
            at = pl.ds(PAD + 8 * c, 8)
            v = V[source, plane, at, :]
            sides = (V[source, plane - 1, at, :] + V[source, plane + 1, at, :]) + (
                V[source, plane, pl.ds(PAD + 8 * c - 1, 8), :]
                + V[source, plane, pl.ds(PAD + 8 * c + 1, 8), :]
            )
            sides = sides + (
                jnp.where(leftmost, 0.0, pltpu.roll(v, 1, 1))
                + jnp.where(rightmost, 0.0, pltpu.roll(v, 127, 1))
            )
            new = D[plane, at, :] * v - scale * sides
            new = 0.5 * new if before is None else new - V[before, plane, at, :]
            V[target, plane, at, :] = new if keep is None else jnp.where(keep, new, 0.0)

    def inner(base, steps, near):
        for j in range(1, steps + 1):
            before = None if j == 1 else base + j - 2

            def pair(i, _, j=j, before=before):
                first = GHOST + near + j + 2 * i
                step(base + j - 1, base + j, before, first)
                step(base + j - 1, base + j, before, first + 1)
                return 0

            lax.fori_loop(0, planes // 2 - near - j, pair, 0)

    def inner_rest(base, steps, near):
        for j in range(1, steps + 1):
            before = None if j == 1 else base + j - 2
            for i in range(j, j + near):
                step(base + j - 1, base + j, before, GHOST + i)
                step(base + j - 1, base + j, before, GHOST + planes - 1 - i)

    def wave(base, steps, g):
        low, high = GHOST - g, GHOST + planes - 1 + g

        def one(j, before):
            keep_low, keep_high = (None, None) if j >= g else (has_below, has_above)
            step(base + j - 1, base + j, before, low + j, keep_low)
            step(base + j - 1, base + j, before, high - j, keep_high)

        for j in range(1, steps + 1):
            one(j, None if j == 1 else base + j - 2)

    pairs = [(i, j) for j in range(STEPS + 1) for i in range(j + 1)]
    place = {pair: i for i, pair in enumerate(pairs)}

    def products(first, last, two, slot):
        mine = [p for p in pairs if first <= p[1] <= last and p != (STEPS, STEPS)]

        def add(plane):
            def some(c, acc):
                acc = list(acc)
                for u in range(4):
                    at = pl.ds(pl.multiple_of(PAD + 32 * c + 8 * u, 8), 8)
                    v = [V[k, plane, at, :] for k in range(last + 1)]
                    for a, (i, j) in enumerate(mine):
                        acc[a] = acc[a] + v[i] * v[j]
                return tuple(acc)

            return some

        acc = tuple(zero for _ in mine)
        for plane in two:
            acc = lax.fori_loop(0, chunks // 4, add(plane), acc)
        for value, pair in zip(acc, mine):
            ACC[place[pair], slot] = value

    def middle_products(first, last, near):
        def one(slot, _):
            at = GHOST + near + 2 * slot
            products(first, last, (at, at + 1), slot)
            return 0

        lax.fori_loop(0, planes // 2 - near, one, 0)

    def side_products(first, last, start, stop):
        def one(i, _):
            products(first, last, (GHOST + i, GHOST + planes - 1 - i), planes // 2 - 1 - i)
            return 0

        lax.fori_loop(start, stop, one, 0)

    def reduce(where, count):
        for pair, lanes in where.items():
            value = (ACC[place[pair], 0], zero)
            for slot in range(1, SLOTS):
                s, e = two_sum(value[0], ACC[place[pair], slot])
                value = (s, value[1] + e)
            for n in lanes:
                RED[0, 8 * n : 8 * n + 8, :] = value[0]
                RED[1, 8 * n : 8 * n + 8, :] = value[1]
        for q in range(16):
            if 8 * q >= count:
                PACK[0, 8 * q : 8 * q + 8, :] = zero
                PACK[1, 8 * q : 8 * q + 8, :] = zero
                continue
            total = tree2(
                [
                    tuple(RED[h, pl.ds(64 * q + s, 8, stride=8), :] for h in range(2))
                    for s in range(8)
                ]
            )
            PACK[0, 8 * q : 8 * q + 8, :] = total[0]
            PACK[1, 8 * q : 8 * q + 8, :] = total[1]
        high, low = jnp.transpose(PACK[0]), jnp.transpose(PACK[1])
        total = sublanes2(
            tree2([(high[8 * q : 8 * q + 8], low[8 * q : 8 * q + 8]) for q in range(16)])
        )
        return total

    def spread(k, o):
        return pltpu.make_async_remote_copy(
            src_ref=SEND.at[k],
            dst_ref=GOT.at[k, me],
            send_sem=all_send.at[k],
            recv_sem=all_recv.at[k],
            device_id={"slab": lax.rem(me + o, devices)},
            device_id_type=MESH,
        )

    def share(k, total):
        SEND[k, 0:1, :] = total[0][0:1]
        SEND[k, 1:2, :] = total[1][0:1]
        GOT[k, me, 0:1, :] = total[0][0:1]
        GOT[k, me, 1:2, :] = total[1][0:1]
        for o in range(1, devices):
            spread(k, o).start()

    def wait_shared():
        for k in range(2):
            sent = GOT.at[k, pl.ds(0, devices - 1)]
            pltpu.make_async_copy(sent, sent, all_send.at[k]).wait()

    def wait_row(k):
        arrived = GOT.at[k, pl.ds(0, devices - 1)]
        pltpu.make_async_copy(arrived, arrived, all_recv.at[k]).wait()

    def collect(k):
        wait_row(k)
        value = (GOT[k, 0], jnp.zeros((2, 128), jnp.float32))
        for d in range(1, devices):
            s, e = two_sum(value[0], GOT[k, d])
            value = (s, value[1] + e)
        high = jnp.broadcast_to(value[0][0:1], (8, 128))
        low = jnp.broadcast_to(value[1][0:1] + value[0][1:2], (8, 128))
        return quick(high, low)

    for copy in loads[:4]:
        copy.wait()
    pl.semaphore_wait(barrier, devices - 1)
    send(0, "v", 0)
    scale_diag(GHOST, deep)
    scale_diag(GHOST + planes - deep, deep)
    for which, kind, plane in order[1:]:
        if which == 0:
            send(0, kind, plane)
    for copy in loads[4:]:
        copy.wait()
    scale_diag(GHOST + deep, planes - 2 * deep)

    n = STEPS

    def begin(index):
        base, steps, near = BASES[index], BLOCKS[index], BLOCKS[index - 1] if index else 0
        final = index + 1 == len(BLOCKS)
        inner(base, steps, near)
        if final:
            middle_products(base + 1, n - 2, near + steps - 2)
            middle_products(n - 1, n - 1, near + steps - 1)
            middle_products(n, n, near + steps)
        else:
            middle_products(base + 1 if index else 0, base + steps, near + steps)

    begin(0)
    for index, (base, steps) in enumerate(zip(BASES, BLOCKS)):
        final = index + 1 == len(BLOCKS)
        after = 0 if final else BLOCKS[index + 1]
        if index:
            near = BLOCKS[index - 1]
            for which, kind, plane in order:
                if which == index and kind == "d":
                    send(index, kind, plane)
            inner_rest(base, steps, near)
            for plane in range(steps, after):
                send(index + 1, "v", plane)
            side_products(BASES[index - 1] + 1 if index > 1 else 0, base, 0, near)
            if final:
                side_products(base + 1, n - 2, steps - 2, steps - 2 + near)
                side_products(n - 1, n - 1, steps - 1, steps - 1 + near)
                side_products(n, n, steps, steps + near)
            else:
                side_products(base + 1, base + steps, steps, steps + near)
                begin(index + 1)
        for g in range(1, steps + 1):
            receive(index, "v", g - 1)
            if g > 1 and ("d", g - 2) in numbers:
                which = order[numbers[("d", g - 2)]][0]
                if which == index or (index > 0 and which == index - 1 and g - 1 >= BLOCKS[index - 1]):
                    receive(which, "d", g - 2)
            wave(base, steps, g)
            if index == 0:
                if steps - g < after:
                    send(1, "v", steps - g)
                if g == 1:
                    for plane in range(steps, after):
                        send(1, "v", plane)
                    begin(1)
            if final:
                for back, rows_at in ((2, (base + 1, n - 2)), (1, (n - 1, n - 1)), (0, (n, n))):
                    near = steps - back - g
                    if near >= 0:
                        products(
                            *rows_at,
                            (GHOST + near, GHOST + planes - 1 - near),
                            planes // 2 - 1 - near,
                        )
                if g == steps - 2:
                    m = n - 1
                    where = {
                        (i, j): sorted({m * i + j, m * j + i}) for i, j in pairs if j < m
                    }
                    share(0, reduce(where, m * m))
        if index:
            for plane in range(min(steps, after)):
                send(index + 1, "v", plane)
    late = {(i, n - 1): [i] for i in range(n)}
    late.update({(i, n): [LATE + i] for i in range(n)})
    share(1, reduce(late, LATE + n))
    wait_sent()
    wait_shared()

    table_load.wait()
    m = n - 1
    sub = lax.broadcasted_iota(jnp.int32, (8, 128), 0)
    row = lax.broadcasted_iota(jnp.int32, (16, 128), 0)
    wide = lax.broadcasted_iota(jnp.int32, (16, 128), 1)
    got = collect(0)
    parts = []
    for h in range(2):
        top, bottom = zero, zero
        for i in range(m):
            moved = got[h] if i == 0 else pltpu.roll(got[h], 128 - m * i, 1)
            if i < 8:
                top = jnp.where(sub == i, moved, top)
            else:
                bottom = jnp.where(sub == i - 8, moved, bottom)
        both = jnp.concatenate([top, bottom], axis=0)
        parts.append(jnp.where(wide < m, both, TAB[h, 0:16, :]))
    M = tuple(parts)
    for k in range(m):
        column = tuple(jnp.broadcast_to(v[:, k : k + 1], (16, 128)) for v in M)
        pivot = tuple(jnp.broadcast_to(c[k : k + 1, :], (16, 128)) for c in column)
        scaled = mul2(tuple(jnp.broadcast_to(v[k : k + 1, :], (16, 128)) for v in M), inverse2(pivot))
        rest = add2(M, neg2(mul2(column, scaled)))
        M = tuple(jnp.where(row == k, s, v) for s, v in zip(scaled, rest))
    M = tuple(jnp.where(row < m, v, 0.0) for v in M)
    got = collect(1)

    def down(pair, lane0):
        return tuple(
            jnp.broadcast_to(
                jnp.sum(
                    jnp.where(
                        jnp.logical_and(wide == row + lane0, row < m),
                        jnp.concatenate([v, v], axis=0),
                        0.0,
                    ),
                    axis=1,
                    keepdims=True,
                ),
                (16, 128),
            )
            for v in pair
        )

    def over_rows(pair):
        return sublanes2(add2(tuple(t[0:8] for t in pair), tuple(t[8:16] for t in pair)))

    def at_lane(pair, k):
        return tuple(jnp.broadcast_to(t[:, k : k + 1], (8, 128)) for t in pair)

    near_last, last_column = down(got, 0), down(got, LATE)
    corner, side = at_lane(got, m), at_lane(got, LATE + m)
    first, second = over_rows(mul2(M, near_last)), over_rows(mul2(M, last_column))
    image = down(first, WHOLE)
    pivot = add2(corner, neg2(over_rows(mul2(image, near_last))))
    value = add2(side, neg2(over_rows(mul2(image, last_column))))
    share_last = mul2(value, inverse2(pivot))
    edge = add2(tuple(TAB[h, 16:24, :] for h in range(2)), neg2(first))
    terms = add2(tuple(TAB[h, 24:32, :] for h in range(2)), neg2(second))
    terms = add2(terms, neg2(mul2(edge, share_last)))
    terms = mul2(terms, inverse2(at_lane(terms, SHIFT + 2 * n + 1)))
    factor = terms[0]
    for i in range(2 * n + 1):
        COEF[i] = jnp.broadcast_to(factor[:, SHIFT + i : SHIFT + i + 1], (8, 128))


def combine_kernel(V, COEF, x_out, r_out, X, R, sem):
    planes, rows = X.shape[0], X.shape[1]
    n = STEPS
    fx = [COEF[i] for i in range(n)]
    fr = [COEF[n + i] for i in range(n + 1)]

    def one(i, _):
        for c in range(rows // 8):
            at = pl.ds(8 * c, 8)
            v = [V[k, GHOST + i, pl.ds(PAD + 8 * c, 8), :] for k in range(n + 1)]
            X[i, at, :] = functools.reduce(jnp.add, [f * u for f, u in zip(fx, v)])
            R[i, at, :] = functools.reduce(jnp.add, [f * u for f, u in zip(fr, v)])
        return 0

    copies = []
    group = 2
    for q in range(planes // group):
        lax.fori_loop(group * q, group * q + group, one, 0)
        at = pl.ds(group * q, group)
        for k, (source, target) in enumerate(((X, x_out), (R, r_out))):
            copies.append(pltpu.make_async_copy(source.at[at], target.at[at], sem.at[k, q]))
            copies[-1].start()
    for copy in copies:
        copy.wait()


def local(right_side, diagonal):
    planes, rows, lanes = right_side.shape
    devices = lax.axis_size("slab")
    tall = planes + 2 * GHOST
    f32 = jnp.float32
    out = jax.ShapeDtypeStruct(right_side.shape, f32)
    held = (
        pltpu.VMEM((STEPS + 1, tall, rows + 2 * PAD, lanes), f32),
        pltpu.VMEM((2 * STEPS + 1, 8, 128), f32),
    )
    dma = pltpu.SemaphoreType.DMA
    results = pl.pallas_call(
        functools.partial(kernel, devices),
        out_shape=held,
        in_specs=[pl.BlockSpec(memory_space=pltpu.HBM)] * 3,
        out_specs=(pl.BlockSpec(memory_space=pltpu.VMEM),) * 2,
        scratch_shapes=[
            pltpu.VMEM((tall, rows + 2 * PAD, lanes), f32),
            pltpu.VMEM(((STEPS + 1) * (STEPS + 2) // 2, SLOTS, 8, 128), f32),
            pltpu.VMEM((2, 1024, 128), f32),
            pltpu.VMEM((2, 128, 128), f32),
            pltpu.VMEM((2, 2, 128), f32),
            pltpu.VMEM((2, devices, 2, 128), f32),
            pltpu.VMEM((2, 32, 128), f32),
            dma((7,)),
            dma((2,)),
            dma((2, MESSAGES)),
            dma((2,)),
            dma((2,)),
        ],
        compiler_params=pltpu.CompilerParams(
            collective_id=0, has_side_effects=True, vmem_limit_bytes=16 * 2**20
        ),
        name="cg",
    )(
        *(
            pltpu.with_memory_space_constraint(a, pltpu.HBM)
            for a in (right_side, diagonal, jnp.asarray(tables()))
        )
    )
    return pl.pallas_call(
        combine_kernel,
        out_shape=(out, out),
        in_specs=[pl.BlockSpec(memory_space=pltpu.VMEM)] * 2,
        out_specs=(pl.BlockSpec(memory_space=pltpu.HBM),) * 2,
        scratch_shapes=[
            pltpu.VMEM(right_side.shape, f32),
            pltpu.VMEM(right_side.shape, f32),
            dma((2, planes // 2)),
        ],
        compiler_params=pltpu.CompilerParams(vmem_limit_bytes=8 * 2**20),
        name="combine",
    )(*(pltpu.with_memory_space_constraint(a, pltpu.VMEM) for a in results))


def solution(mesh):
    placed = (P("slab", "sys", None), P("slab", "sys", None))
    return jax.shard_map(
        local,
        mesh=mesh,
        in_specs=placed,
        out_specs=placed,
        check_vma=False,
    )
```

```python
import functools

import jax
import jax.numpy as jnp
import numpy as np
from jax import lax
from jax.experimental import pallas as pl
from jax.experimental.pallas import tpu as pltpu
from jax.sharding import PartitionSpec as P

MID = 7.125
HALF = 6.875
BLOCKS = (3, 3, 4)
STEPS = sum(BLOCKS)
BASES = tuple(int(b) for b in np.cumsum((0,) + BLOCKS[:-1]))
GHOST = max(BLOCKS)
MESSAGES = STEPS + GHOST - 1
PAD = 8
SLOTS = 8
SHIFT = 32
WHOLE = 64
LATE = 16
MESH = pl.DeviceIdType.MESH


def tables():
    n = STEPS
    apply = np.zeros((n + 1, n))
    at_zero = np.zeros(n + 1)
    at_zero[0] = 1.0
    for base, steps in zip(BASES, BLOCKS):
        for j in range(steps):
            i = base + j
            apply[i, i] = MID
            if j == 0:
                apply[i + 1, i] = HALF
                at_zero[i + 1] = -MID / HALF * at_zero[i]
            else:
                apply[i + 1, i] = apply[i - 1, i] = HALF / 2
                at_zero[i + 1] = -2 * MID / HALF * at_zero[i] - at_zero[i - 1]
    divide = np.zeros((n, n + 1))
    divide[:, 1:] = -np.linalg.inv(apply[1:])
    maps = np.concatenate([divide, np.eye(n + 1), at_zero[None]]).T
    sides = np.zeros((32, 128))
    wide = slice(SHIFT, SHIFT + maps.shape[1])
    sides[: n - 1, wide] = maps[: n - 1]
    sides[: n - 1, WHOLE : WHOLE + n - 1] = np.eye(n - 1)
    sides[16:24, wide] = maps[n - 1]
    sides[24:, wide] = maps[n]
    high = sides.astype(np.float32)
    return np.stack([high, (sides - high).astype(np.float32)])


def two_sum(a, b):
    s = a + b
    t = s - a
    return s, (a - (s - t)) + (b - t)


def quick(a, b):
    s = a + b
    return s, b - (s - a)


def halves(a):
    c = a * 4097.0
    h = c - (c - a)
    return h, a - h


def add2(a, b):
    s, e = two_sum(a[0], b[0])
    return quick(s, e + (a[1] + b[1]))


def mul2(a, b):
    p = a[0] * b[0]
    ah, al = halves(a[0])
    bh, bl = halves(b[0])
    e = ((ah * bh - p) + (ah * bl + al * bh)) + al * bl
    return quick(p, e + (a[0] * b[1] + a[1] * b[0]))


def neg2(a):
    return (-a[0], -a[1])


def inverse2(a):
    y = 1.0 / a[0]
    zero = jnp.zeros_like(y)
    p, e = mul2(a, (y, zero))
    return quick(y, y * ((1.0 - p) - e))


def tree2(parts):
    while len(parts) > 1:
        parts = [add2(parts[i], parts[i + 1]) for i in range(0, len(parts) - 1, 2)] + (
            [parts[-1]] if len(parts) % 2 else []
        )
    return parts[0]


def sublanes2(a):
    for shift in (4, 2, 1):
        a = add2(a, tuple(pltpu.roll(v, shift, 0) for v in a))
    return a


def kernel(
    devices,
    right_ref,
    diag_ref,
    table_ref,
    V,
    COEF,
    D,
    ACC,
    RED,
    PACK,
    SEND,
    GOT,
    TAB,
    load_sem,
    send_sem,
    recv_sem,
    all_send,
    all_recv,
):
    planes, rows = right_ref.shape[0], right_ref.shape[1]
    chunks = rows // 8
    me = lax.axis_index("slab")
    below = lax.rem(me + devices - 1, devices)
    above = lax.rem(me + 1, devices)
    has_below = me > 0
    has_above = me < devices - 1
    body = pl.ds(PAD, rows)
    deep = GHOST

    def load(ref, at, first, count, sem):
        return pltpu.make_async_copy(
            ref.at[pl.ds(first, count)], at.at[pl.ds(GHOST + first, count), body], load_sem.at[sem]
        )

    loads = []
    for sem, (ref, at) in enumerate(((right_ref, V.at[0]), (diag_ref, D))):
        loads.append(load(ref, at, 0, deep, 3 * sem))
        loads.append(load(ref, at, planes - deep, deep, 3 * sem + 1))
    for sem, (ref, at) in enumerate(((right_ref, V.at[0]), (diag_ref, D))):
        loads.append(load(ref, at, deep, planes - 2 * deep, 3 * sem + 2))
    table_load = pltpu.make_async_copy(table_ref, TAB, load_sem.at[6])
    for copy in loads:
        copy.start()
    table_load.start()

    barrier = pltpu.get_barrier_semaphore()
    for o in range(1, devices):
        pl.semaphore_signal(
            barrier, inc=1, device_id={"slab": lax.rem(me + o, devices)}, device_id_type=MESH
        )

    zero = jnp.zeros((8, 128), jnp.float32)

    def clear(i, _):
        for k in range(STEPS):
            V[k, i, 0:8, :] = zero
            V[k, i, PAD + rows : PAD + rows + 8, :] = zero
        return 0

    lax.fori_loop(0, planes + 2 * GHOST, clear, 0)

    def clear_ghost(first):
        for base in BASES:
            for i in range(GHOST):
                for c in range(chunks):
                    V[base, first + i, PAD + 8 * c : PAD + 8 * c + 8, :] = zero

    @pl.when(jnp.logical_not(has_below))
    def _():
        clear_ghost(0)

    @pl.when(jnp.logical_not(has_above))
    def _():
        clear_ghost(GHOST + planes)

    def message(array, plane, up, t):
        if up:
            source, target = GHOST + planes - 1 - plane, GHOST - 1 - plane
        else:
            source, target = GHOST + plane, GHOST + planes + plane
        return pltpu.make_async_remote_copy(
            src_ref=array.at[source, body],
            dst_ref=array.at[target, body],
            send_sem=send_sem.at[int(up)],
            recv_sem=recv_sem.at[int(up), t],
            device_id={"slab": above if up else below},
            device_id_type=MESH,
        )

    numbers = {}
    order = []
    diag_sent = 0
    for index, (base, steps) in enumerate(zip(BASES, BLOCKS)):
        for plane in range(steps):
            order.append((index, "v", plane))
            if index == 0 and plane < steps - 1:
                order.append((index, "d", plane))
        upto = steps - 1 if index + 1 == len(BLOCKS) else max(BLOCKS[: index + 2]) - 1
        for plane in range(max(diag_sent, BLOCKS[0] - 1), upto):
            order.append((index, "d", plane))
        diag_sent = max(upto, diag_sent, BLOCKS[0] - 1)
    for t, (index, kind, plane) in enumerate(order):
        numbers[(kind, plane) if kind == "d" else (kind, index, plane)] = t

    def of(index, kind, plane, up):
        t = numbers[(kind, plane) if kind == "d" else (kind, index, plane)]
        return message(D if kind == "d" else V.at[BASES[index]], plane, up, t)

    def send(index, kind, plane):
        @pl.when(has_below)
        def _():
            of(index, kind, plane, False).start()

        @pl.when(has_above)
        def _():
            of(index, kind, plane, True).start()

    def wait_sent():
        for up, there in ((False, has_below), (True, has_above)):

            @pl.when(there)
            def _(up=up):
                sent = D.at[pl.ds(0, len(order)), body]
                pltpu.make_async_copy(sent, sent, send_sem.at[int(up)]).wait()

    def receive(index, kind, plane):
        @pl.when(has_below)
        def _():
            of(index, kind, plane, True).wait_recv()

        @pl.when(has_above)
        def _():
            of(index, kind, plane, False).wait_recv()

    lane = lax.broadcasted_iota(jnp.int32, (8, 128), 1)
    leftmost, rightmost = lane == 0, lane == 127
    scale = np.float32(2.0 / HALF)

    def scale_diag(first, count):
        def one(i, _):
            for c in range(chunks):
                at = pl.ds(PAD + 8 * c, 8)
                D[first + i, at, :] = (D[first + i, at, :] + np.float32(6.0 - MID)) * scale
            return 0

        lax.fori_loop(0, count, one, 0)

    def step(source, target, before, plane, keep=None):
        for c in range(chunks):
            at = pl.ds(PAD + 8 * c, 8)
            v = V[source, plane, at, :]
            sides = (V[source, plane - 1, at, :] + V[source, plane + 1, at, :]) + (
                V[source, plane, pl.ds(PAD + 8 * c - 1, 8), :]
                + V[source, plane, pl.ds(PAD + 8 * c + 1, 8), :]
            )
            sides = sides + (
                jnp.where(leftmost, 0.0, pltpu.roll(v, 1, 1))
                + jnp.where(rightmost, 0.0, pltpu.roll(v, 127, 1))
            )
            new = D[plane, at, :] * v - scale * sides
            new = 0.5 * new if before is None else new - V[before, plane, at, :]
            V[target, plane, at, :] = new if keep is None else jnp.where(keep, new, 0.0)

    def inner(base, steps, near):
        for j in range(1, steps + 1):
            before = None if j == 1 else base + j - 2

            def pair(i, _, j=j, before=before):
                first = GHOST + near + j + 2 * i
                step(base + j - 1, base + j, before, first)
                step(base + j - 1, base + j, before, first + 1)
                return 0

            lax.fori_loop(0, planes // 2 - near - j, pair, 0)

    def inner_rest(base, steps, near):
        for j in range(1, steps + 1):
            before = None if j == 1 else base + j - 2
            for i in range(j, j + near):
                step(base + j - 1, base + j, before, GHOST + i)
                step(base + j - 1, base + j, before, GHOST + planes - 1 - i)

    def wave(base, steps, g):
        low, high = GHOST - g, GHOST + planes - 1 + g

        def one(j, before):
            keep_low, keep_high = (None, None) if j >= g else (has_below, has_above)
            step(base + j - 1, base + j, before, low + j, keep_low)
            step(base + j - 1, base + j, before, high - j, keep_high)

        for j in range(1, steps + 1):
            one(j, None if j == 1 else base + j - 2)

    pairs = [(i, j) for j in range(STEPS + 1) for i in range(j + 1)]
    place = {pair: i for i, pair in enumerate(pairs)}

    def products(first, last, two, slot):
        mine = [p for p in pairs if first <= p[1] <= last and p != (STEPS, STEPS)]

        def add(plane):
            def some(c, acc):
                acc = list(acc)
                for u in range(4):
                    at = pl.ds(pl.multiple_of(PAD + 32 * c + 8 * u, 8), 8)
                    v = [V[k, plane, at, :] for k in range(last + 1)]
                    for a, (i, j) in enumerate(mine):
                        acc[a] = acc[a] + v[i] * v[j]
                return tuple(acc)

            return some

        acc = tuple(zero for _ in mine)
        for plane in two:
            acc = lax.fori_loop(0, chunks // 4, add(plane), acc)
        for value, pair in zip(acc, mine):
            ACC[place[pair], slot] = value

    def middle_products(first, last, near):
        def one(slot, _):
            at = GHOST + near + 2 * slot
            products(first, last, (at, at + 1), slot)
            return 0

        lax.fori_loop(0, planes // 2 - near, one, 0)

    def side_products(first, last, start, stop):
        def one(i, _):
            products(first, last, (GHOST + i, GHOST + planes - 1 - i), planes // 2 - 1 - i)
            return 0

        lax.fori_loop(start, stop, one, 0)

    def reduce(where, count):
        for pair, lanes in where.items():
            value = (ACC[place[pair], 0], zero)
            for slot in range(1, SLOTS):
                s, e = two_sum(value[0], ACC[place[pair], slot])
                value = (s, value[1] + e)
            for n in lanes:
                RED[0, 8 * n : 8 * n + 8, :] = value[0]
                RED[1, 8 * n : 8 * n + 8, :] = value[1]
        for q in range(16):
            if 8 * q >= count:
                PACK[0, 8 * q : 8 * q + 8, :] = zero
                PACK[1, 8 * q : 8 * q + 8, :] = zero
                continue
            total = tree2(
                [
                    tuple(RED[h, pl.ds(64 * q + s, 8, stride=8), :] for h in range(2))
                    for s in range(8)
                ]
            )
            PACK[0, 8 * q : 8 * q + 8, :] = total[0]
            PACK[1, 8 * q : 8 * q + 8, :] = total[1]
        high, low = jnp.transpose(PACK[0]), jnp.transpose(PACK[1])
        total = sublanes2(
            tree2([(high[8 * q : 8 * q + 8], low[8 * q : 8 * q + 8]) for q in range(16)])
        )
        return total

    def spread(k, o):
        return pltpu.make_async_remote_copy(
            src_ref=SEND.at[k],
            dst_ref=GOT.at[k, me],
            send_sem=all_send.at[k],
            recv_sem=all_recv.at[k],
            device_id={"slab": lax.rem(me + o, devices)},
            device_id_type=MESH,
        )

    def share(k, total):
        SEND[k, 0:1, :] = total[0][0:1]
        SEND[k, 1:2, :] = total[1][0:1]
        GOT[k, me, 0:1, :] = total[0][0:1]
        GOT[k, me, 1:2, :] = total[1][0:1]
        for o in range(1, devices):
            spread(k, o).start()

    def wait_shared():
        for k in range(2):
            sent = GOT.at[k, pl.ds(0, devices - 1)]
            pltpu.make_async_copy(sent, sent, all_send.at[k]).wait()

    def wait_row(k):
        arrived = GOT.at[k, pl.ds(0, devices - 1)]
        pltpu.make_async_copy(arrived, arrived, all_recv.at[k]).wait()

    def collect(k):
        wait_row(k)
        value = (GOT[k, 0], jnp.zeros((2, 128), jnp.float32))
        for d in range(1, devices):
            s, e = two_sum(value[0], GOT[k, d])
            value = (s, value[1] + e)
        high = jnp.broadcast_to(value[0][0:1], (8, 128))
        low = jnp.broadcast_to(value[1][0:1] + value[0][1:2], (8, 128))
        return quick(high, low)

    for copy in loads[:4]:
        copy.wait()
    pl.semaphore_wait(barrier, devices - 1)
    send(0, "v", 0)
    scale_diag(GHOST, deep)
    scale_diag(GHOST + planes - deep, deep)
    for which, kind, plane in order[1:]:
        if which == 0:
            send(0, kind, plane)
    for copy in loads[4:]:
        copy.wait()
    scale_diag(GHOST + deep, planes - 2 * deep)

    n = STEPS

    def begin(index):
        base, steps, near = BASES[index], BLOCKS[index], BLOCKS[index - 1] if index else 0
        final = index + 1 == len(BLOCKS)
        inner(base, steps, near)
        if final:
            middle_products(base + 1, n - 2, near + steps - 2)
            middle_products(n - 1, n - 1, near + steps - 1)
            middle_products(n, n, near + steps)
        else:
            middle_products(base + 1 if index else 0, base + steps, near + steps)

    begin(0)
    for index, (base, steps) in enumerate(zip(BASES, BLOCKS)):
        final = index + 1 == len(BLOCKS)
        after = 0 if final else BLOCKS[index + 1]
        if index:
            near = BLOCKS[index - 1]
            for which, kind, plane in order:
                if which == index and kind == "d":
                    send(index, kind, plane)
            inner_rest(base, steps, near)
            for plane in range(steps, after):
                send(index + 1, "v", plane)
            side_products(BASES[index - 1] + 1 if index > 1 else 0, base, 0, near)
            if final:
                side_products(base + 1, n - 2, steps - 2, steps - 2 + near)
                side_products(n - 1, n - 1, steps - 1, steps - 1 + near)
                side_products(n, n, steps, steps + near)
            else:
                side_products(base + 1, base + steps, steps, steps + near)
                begin(index + 1)
        for g in range(1, steps + 1):
            receive(index, "v", g - 1)
            if g > 1 and ("d", g - 2) in numbers:
                which = order[numbers[("d", g - 2)]][0]
                if which == index or (index > 0 and which == index - 1 and g - 1 >= BLOCKS[index - 1]):
                    receive(which, "d", g - 2)
            wave(base, steps, g)
            if index == 0:
                if steps - g < after:
                    send(1, "v", steps - g)
                if g == 1:
                    for plane in range(steps, after):
                        send(1, "v", plane)
                    begin(1)
            if final:
                for back, rows_at in ((2, (base + 1, n - 2)), (1, (n - 1, n - 1)), (0, (n, n))):
                    near = steps - back - g
                    if near >= 0:
                        products(
                            *rows_at,
                            (GHOST + near, GHOST + planes - 1 - near),
                            planes // 2 - 1 - near,
                        )
                if g == steps - 2:
                    m = n - 1
                    where = {
                        (i, j): sorted({m * i + j, m * j + i}) for i, j in pairs if j < m
                    }
                    share(0, reduce(where, m * m))
        if index:
            for plane in range(min(steps, after)):
                send(index + 1, "v", plane)
    late = {(i, n - 1): [i] for i in range(n)}
    late.update({(i, n): [LATE + i] for i in range(n)})
    share(1, reduce(late, LATE + n))
    wait_sent()
    wait_shared()

    table_load.wait()
    m = n - 1
    sub = lax.broadcasted_iota(jnp.int32, (8, 128), 0)
    row = lax.broadcasted_iota(jnp.int32, (16, 128), 0)
    wide = lax.broadcasted_iota(jnp.int32, (16, 128), 1)
    got = collect(0)
    parts = []
    for h in range(2):
        top, bottom = zero, zero
        for i in range(m):
            moved = got[h] if i == 0 else pltpu.roll(got[h], 128 - m * i, 1)
            if i < 8:
                top = jnp.where(sub == i, moved, top)
            else:
                bottom = jnp.where(sub == i - 8, moved, bottom)
        both = jnp.concatenate([top, bottom], axis=0)
        parts.append(jnp.where(wide < m, both, TAB[h, 0:16, :]))
    M = tuple(parts)
    for k in range(m):
        column = tuple(jnp.broadcast_to(v[:, k : k + 1], (16, 128)) for v in M)
        pivot = tuple(jnp.broadcast_to(c[k : k + 1, :], (16, 128)) for c in column)
        scaled = mul2(tuple(jnp.broadcast_to(v[k : k + 1, :], (16, 128)) for v in M), inverse2(pivot))
        rest = add2(M, neg2(mul2(column, scaled)))
        M = tuple(jnp.where(row == k, s, v) for s, v in zip(scaled, rest))
    M = tuple(jnp.where(row < m, v, 0.0) for v in M)
    got = collect(1)

    def down(pair, lane0):
        return tuple(
            jnp.broadcast_to(
                jnp.sum(
                    jnp.where(
                        jnp.logical_and(wide == row + lane0, row < m),
                        jnp.concatenate([v, v], axis=0),
                        0.0,
                    ),
                    axis=1,
                    keepdims=True,
                ),
                (16, 128),
            )
            for v in pair
        )

    def over_rows(pair):
        return sublanes2(add2(tuple(t[0:8] for t in pair), tuple(t[8:16] for t in pair)))

    def at_lane(pair, k):
        return tuple(jnp.broadcast_to(t[:, k : k + 1], (8, 128)) for t in pair)

    near_last, last_column = down(got, 0), down(got, LATE)
    corner, side = at_lane(got, m), at_lane(got, LATE + m)
    first, second = over_rows(mul2(M, near_last)), over_rows(mul2(M, last_column))
    image = down(first, WHOLE)
    pivot = add2(corner, neg2(over_rows(mul2(image, near_last))))
    value = add2(side, neg2(over_rows(mul2(image, last_column))))
    share_last = mul2(value, inverse2(pivot))
    edge = add2(tuple(TAB[h, 16:24, :] for h in range(2)), neg2(first))
    terms = add2(tuple(TAB[h, 24:32, :] for h in range(2)), neg2(second))
    terms = add2(terms, neg2(mul2(edge, share_last)))
    terms = mul2(terms, inverse2(at_lane(terms, SHIFT + 2 * n + 1)))
    factor = terms[0]
    for i in range(2 * n + 1):
        COEF[i] = jnp.broadcast_to(factor[:, SHIFT + i : SHIFT + i + 1], (8, 128))


def combine_kernel(V, COEF, x_out, r_out, X, R, sem):
    planes, rows = X.shape[0], X.shape[1]
    n = STEPS
    fx = [COEF[i] for i in range(n)]
    fr = [COEF[n + i] for i in range(n + 1)]

    def one(i, _):
        for c in range(rows // 8):
            at = pl.ds(8 * c, 8)
            v = [V[k, GHOST + i, pl.ds(PAD + 8 * c, 8), :] for k in range(n + 1)]
            X[i, at, :] = functools.reduce(jnp.add, [f * u for f, u in zip(fx, v)])
            R[i, at, :] = functools.reduce(jnp.add, [f * u for f, u in zip(fr, v)])
        return 0

    copies = []
    edges = list(range(0, planes - 1, 2)) + [planes - 1, planes]
    for q, (first, last) in enumerate(zip(edges[:-1], edges[1:])):
        lax.fori_loop(first, last, one, 0)
        at = pl.ds(first, last - first)
        for k, (source, target) in enumerate(((X, x_out), (R, r_out))):
            copies.append(pltpu.make_async_copy(source.at[at], target.at[at], sem.at[k, q]))
            copies[-1].start()
    for copy in copies:
        copy.wait()


def local(right_side, diagonal):
    planes, rows, lanes = right_side.shape
    devices = lax.axis_size("slab")
    tall = planes + 2 * GHOST
    f32 = jnp.float32
    out = jax.ShapeDtypeStruct(right_side.shape, f32)
    held = (
        pltpu.VMEM((STEPS + 1, tall, rows + 2 * PAD, lanes), f32),
        pltpu.VMEM((2 * STEPS + 1, 8, 128), f32),
    )
    dma = pltpu.SemaphoreType.DMA
    results = pl.pallas_call(
        functools.partial(kernel, devices),
        out_shape=held,
        in_specs=[pl.BlockSpec(memory_space=pltpu.HBM)] * 3,
        out_specs=(pl.BlockSpec(memory_space=pltpu.VMEM),) * 2,
        scratch_shapes=[
            pltpu.VMEM((tall, rows + 2 * PAD, lanes), f32),
            pltpu.VMEM(((STEPS + 1) * (STEPS + 2) // 2, SLOTS, 8, 128), f32),
            pltpu.VMEM((2, 1024, 128), f32),
            pltpu.VMEM((2, 128, 128), f32),
            pltpu.VMEM((2, 2, 128), f32),
            pltpu.VMEM((2, devices, 2, 128), f32),
            pltpu.VMEM((2, 32, 128), f32),
            dma((7,)),
            dma((2,)),
            dma((2, MESSAGES)),
            dma((2,)),
            dma((2,)),
        ],
        compiler_params=pltpu.CompilerParams(
            collective_id=0, has_side_effects=True, vmem_limit_bytes=16 * 2**20
        ),
        name="cg",
    )(
        *(
            pltpu.with_memory_space_constraint(a, pltpu.HBM)
            for a in (right_side, diagonal, jnp.asarray(tables()))
        )
    )
    return pl.pallas_call(
        combine_kernel,
        out_shape=(out, out),
        in_specs=[pl.BlockSpec(memory_space=pltpu.VMEM)] * 2,
        out_specs=(pl.BlockSpec(memory_space=pltpu.HBM),) * 2,
        scratch_shapes=[
            pltpu.VMEM(right_side.shape, f32),
            pltpu.VMEM(right_side.shape, f32),
            dma((2, planes // 2 + 1)),
        ],
        compiler_params=pltpu.CompilerParams(vmem_limit_bytes=8 * 2**20),
        name="combine",
    )(*(pltpu.with_memory_space_constraint(a, pltpu.VMEM) for a in results))


def solution(mesh):
    placed = (P("slab", "sys", None), P("slab", "sys", None))
    return jax.shard_map(
        local,
        mesh=mesh,
        in_specs=placed,
        out_specs=placed,
        check_vma=False,
    )
```
